32 devices in a mesh: job: 4 (over y, x), dp: 2 (over core), tp: 4 (over z).
Axes of the slice: x: 2, y: 2, z: 4, core: 2. Of those that a mesh axis runs over, the one named last changes fastest.
Arguments:
- partial_up: float32 [8, 768, 3072], P(('job', 'dp'), None, 'tp'), parts along dimension 0, may hold values from -0.875 to 0.875
- partial_down: float32 [8, 3072, 768], P(('job', 'dp'), 'tp'), parts along dimension 0, may hold values from -0.875 to 0.875
- partial_norm: float32 [8, 768], P(('job', 'dp')), parts along dimension 0, may hold values from -8 to 8
- partial_bias: float32 [8, 768], P(('job', 'dp')), parts along dimension 0, may hold values from -8 to 8
- master_up: float32 [3072, 3072], P(('job', 'dp'), 'tp'), parts along dimension 0, may hold values from -0.3125 to 0.3125
- master_down: float32 [12288, 768], P(('job', 'tp'), 'dp'), parts along dimension 0, may hold values from -0.15625 to 0.15625
- master_norm: float32 [3072], P(('job', 'dp')), parts along dimension 0, may hold values from 0.25 to 1.75
- master_bias: float32 [3072], P(('job', 'dp')), parts along dimension 0, may hold values from -3 to 3
- memory_up: float32 [3072, 3072], P(('job', 'dp'), 'tp'), parts along dimension 0, may hold values from -0.21875 to 0.21875
- memory_down: float32 [12288, 768], P(('job', 'tp'), 'dp'), parts along dimension 0, may hold values from -0.109375 to 0.109375
- memory_norm: float32 [3072], P(('job', 'dp')), parts along dimension 0, may hold values from -1.75 to 1.75
- memory_bias: float32 [3072], P(('job', 'dp')), parts along dimension 0, may hold values from -1.75 to 1.75
Outputs:
- compute_up: bfloat16 [3072, 3072], P('job', 'tp'), parts along dimension 0
- compute_down: bfloat16 [12288, 768], P(('job', 'tp')), parts along dimension 0
- compute_norm: bfloat16 [3072], P('job'), parts along dimension 0
- compute_bias: bfloat16 [3072], P('job'), parts along dimension 0
- stepped_up: float32 [3072, 3072], P(('job', 'dp'), 'tp'), parts along dimension 0
- stepped_down: float32 [12288, 768], P(('job', 'tp'), 'dp'), parts along dimension 0
- stepped_norm: float32 [3072], P(('job', 'dp')), parts along dimension 0
- stepped_bias: float32 [3072], P(('job', 'dp')), parts along dimension 0
- state_new_up: float32 [3072, 3072], P(('job', 'dp'), 'tp'), parts along dimension 0
- state_new_down: float32 [12288, 768], P(('job', 'tp'), 'dp'), parts along dimension 0
- state_new_norm: float32 [3072], P(('job', 'dp')), parts along dimension 0
- state_new_bias: float32 [3072], P(('job', 'dp')), parts along dimension 0
The draws below stay inside these ranges and needn't reach their ends.
There are 4 independent parts, one for each index of `job`. The reference program is written for one: setup_inputs(seed, part) draws one part's arguments, and reference() takes and returns one part's arrays. A program takes and returns all parts, laid end to end along the dimension named above; each array names one. Nothing has to cross between parts.
All inputs are finite; a program needn't handle non-finite values.
Results may differ from the reference program's by a relative error of at most 0.001.
Values may be sent and summed in bfloat16 or wider, within the bound.
A program may use at most 64 MiB of HBM per device.

```python
import jax
import jax.numpy as jnp
from jax import lax

WIDTH = 768
INNER = 3072
REPLICAS = 2


def with_spikes(values, key, source, target, shards_of, factor):
    owner, partner = [(jnp.arange(values.shape[axis_at]) // (values.shape[axis_at] // shards_of)).reshape([-1 if axis == axis_at else 1 for axis in range(values.ndim)]) for axis_at in (source, target)]
    chosen = jax.random.permutation(key, shards_of)[partner]
    strong = (owner == chosen) | (owner == (partner + shards_of // 2) % shards_of)
    return jnp.where(strong, factor * values, values)


def levels(key, shape, split, smallest, largest):
    level, own = 1.0, jax.random.fold_in(key, 6)
    for dim, parts in split:
        draws = jnp.exp(jax.random.uniform(jax.random.fold_in(own, dim), (parts,), jnp.float32, smallest / len(split), largest / len(split)))
        level = level * jnp.repeat(draws, shape[dim] // parts).reshape([-1 if axis == dim else 1 for axis in range(len(shape))])
    return level


def bell_draw(stream_key, dims, width, most, shards=(), held_as=jnp.bfloat16):
    entries = jax.random.normal(stream_key, dims, jnp.float32) * width
    if len(shards) > 0:
        entries = levels(stream_key, dims, shards, -0.22, 0.18) * entries
    return jnp.clip(entries, min=-most, max=most).astype(held_as)


def heavy_noise(rng, dims, deviation, most, cuts, heavy, kind=jnp.bfloat16):
    values = deviation * jax.random.normal(rng, dims, jnp.float32)
    if cuts:
        values = values * levels(rng, dims, cuts, -0.22, 0.18)
    return jnp.clip(with_spikes(values, jax.random.fold_in(rng, 3), *heavy), -most, most).astype(kind)


def setup_inputs(seed: int = 0, part: int = 0) -> dict:
    key_list = jax.random.split(jax.random.key(seed), 13)
    part_splits = jax.random.split(jax.random.fold_in(key_list[12], part), 13)
    return {
        "partial_up": heavy_noise(part_splits[0], (REPLICAS, WIDTH, INNER), 0.1, 0.875, ((0, 2), (2, 4)), (0, 1, 2, 2.0), jnp.float32),
        "partial_down": heavy_noise(part_splits[1], (REPLICAS, INNER, WIDTH), 0.1, 0.875, ((0, 2), (1, 4)), (0, 2, 2, 2.0), jnp.float32),
        "partial_norm": heavy_noise(part_splits[2], (REPLICAS, WIDTH), 1.0, 8.0, ((0, 2),), (0, 1, 2, 2.0), jnp.float32),
        "partial_bias": heavy_noise(part_splits[3], (REPLICAS, WIDTH), 1.0, 8.0, ((0, 2),), (0, 1, 2, 2.0), jnp.float32),
        "master_up": heavy_noise(part_splits[4], (WIDTH, INNER), WIDTH ** -0.5, 0.3125, ((0, 2), (1, 4)), (1, 0, 4, 2.0), jnp.float32),
        "master_down": heavy_noise(part_splits[5], (INNER, WIDTH), INNER ** -0.5, 0.15625, ((0, 4), (1, 2)), (0, 1, 4, 2.0), jnp.float32),
        "master_norm": jnp.clip(1.0 + 0.15 * jax.random.normal(part_splits[6], (WIDTH,), jnp.float32), 0.25, 1.75),
        "master_bias": bell_draw(part_splits[7], (WIDTH,), 0.5, 3.0, ((0, 2),), jnp.float32),
        "memory_up": bell_draw(part_splits[8], (WIDTH, INNER), WIDTH ** -0.5, 0.21875, ((0, 2), (1, 4)), jnp.float32),
        "memory_down": bell_draw(part_splits[9], (INNER, WIDTH), INNER ** -0.5, 0.109375, ((0, 4), (1, 2)), jnp.float32),
        "memory_norm": bell_draw(part_splits[10], (WIDTH,), 0.3, 1.75, ((0, 2),), jnp.float32),
        "memory_bias": bell_draw(part_splits[11], (WIDTH,), 0.3, 1.75, ((0, 2),), jnp.float32),
    }


learn_rate = 0.4
hold_rate = 0.9

def reference(partial_up, partial_down, partial_norm, partial_bias, master_up, master_down, master_norm, master_bias, memory_up, memory_down, memory_norm, memory_bias):
    mean_up = lax.optimization_barrier(jnp.sum(partial_up.astype(jnp.float32), axis=0)) * REPLICAS ** (-0.5)
    mean_down = lax.optimization_barrier(jnp.sum(partial_down.astype(jnp.float32), axis=0)) * REPLICAS ** (-0.5)
    mean_norm = lax.optimization_barrier(jnp.sum(partial_norm.astype(jnp.float32), axis=0)) * REPLICAS ** (-0.5)
    mean_bias = lax.optimization_barrier(jnp.sum(partial_bias.astype(jnp.float32), axis=0)) * REPLICAS ** (-0.5)
    ratio_up = jnp.sqrt(lax.optimization_barrier(jnp.sum(master_up * master_up, axis=1, keepdims=True))) * lax.rsqrt(lax.optimization_barrier(jnp.sum(mean_up * mean_up, axis=1, keepdims=True)) + 1e-06)
    mean_up = mean_up * ratio_up
    ratio_down = jnp.sqrt(lax.optimization_barrier(jnp.sum(master_down * master_down, axis=0, keepdims=True))) * lax.rsqrt(lax.optimization_barrier(jnp.sum(mean_down * mean_down, axis=0, keepdims=True)) + 1e-06)
    mean_down = mean_down * ratio_down
    state_new_up = hold_rate * memory_up + mean_up
    stepped_up = master_up - learn_rate * state_new_up
    state_new_down = hold_rate * memory_down + mean_down
    stepped_down = master_down - learn_rate * state_new_down
    state_new_norm = hold_rate * memory_norm + mean_norm
    stepped_norm = master_norm - learn_rate * state_new_norm
    state_new_bias = hold_rate * memory_bias + mean_bias
    stepped_bias = master_bias - learn_rate * state_new_bias
    compute_up = stepped_up.astype(jnp.bfloat16)
    compute_down = stepped_down.astype(jnp.bfloat16)
    compute_norm = stepped_norm.astype(jnp.bfloat16)
    compute_bias = stepped_bias.astype(jnp.bfloat16)
    return (compute_up, compute_down, compute_norm, compute_bias, stepped_up, stepped_down, stepped_norm, stepped_bias, state_new_up, state_new_down, state_new_norm, state_new_bias)
```

```python
import functools

import jax
import jax.numpy as jnp
from jax import lax
from jax.experimental import pallas as pl
from jax.experimental.pallas import tpu as pltpu
from jax.sharding import PartitionSpec as P

learn_rate = 0.4
hold_rate = 0.9


def on_device(
    partial_up,
    partial_down,
    partial_norm,
    partial_bias,
    master_up,
    master_down,
    master_norm,
    master_bias,
    memory_up,
    memory_down,
    memory_norm,
    memory_bias,
):
    mean_up, mean_down = (
        lax.psum_scatter(partial_up[0], "dp", scatter_dimension=0, tiled=True),
        lax.psum_scatter(partial_down[0], "dp", scatter_dimension=1, tiled=True),
    )
    whole_norm, whole_bias = lax.psum((partial_norm[0], partial_bias[0]), "dp")
    place = lax.axis_index("dp")
    mean_norm = lax.dynamic_slice_in_dim(
        whole_norm, place * master_norm.shape[0], master_norm.shape[0]
    )
    mean_bias = lax.dynamic_slice_in_dim(
        whole_bias, place * master_bias.shape[0], master_bias.shape[0]
    )
    mean_rate = lax.axis_size("dp") ** (-0.5)
    mean_up = mean_up * mean_rate
    mean_down = mean_down * mean_rate
    mean_norm = mean_norm * mean_rate
    mean_bias = mean_bias * mean_rate
    own_up, own_down, slope_up_norm, slope_down_norm = lax.psum(
        (
            jnp.sum(master_up * master_up, axis=1, keepdims=True),
            jnp.sum(master_down * master_down, axis=0, keepdims=True),
            jnp.sum(mean_up * mean_up, axis=1, keepdims=True),
            jnp.sum(mean_down * mean_down, axis=0, keepdims=True),
        ),
        "tp",
    )
    mean_up = mean_up * (jnp.sqrt(own_up) * lax.rsqrt(slope_up_norm + 1e-06))
    mean_down = mean_down * (jnp.sqrt(own_down) * lax.rsqrt(slope_down_norm + 1e-06))
    state_new_up = hold_rate * memory_up + mean_up
    stepped_up = master_up - learn_rate * state_new_up
    state_new_down = hold_rate * memory_down + mean_down
    stepped_down = master_down - learn_rate * state_new_down
    state_new_norm = hold_rate * memory_norm + mean_norm
    stepped_norm = master_norm - learn_rate * state_new_norm
    state_new_bias = hold_rate * memory_bias + mean_bias
    stepped_bias = master_bias - learn_rate * state_new_bias
    compute_up, compute_down, compute_norm, compute_bias = (
        lax.all_gather(stepped_up.astype(jnp.bfloat16), "dp", axis=0, tiled=True),
        lax.all_gather(stepped_down.astype(jnp.bfloat16), "dp", axis=1, tiled=True),
        lax.all_gather(stepped_norm.astype(jnp.bfloat16), "dp", axis=0, tiled=True),
        lax.all_gather(stepped_bias.astype(jnp.bfloat16), "dp", axis=0, tiled=True),
    )
    return (
        compute_up,
        compute_down,
        compute_norm,
        compute_bias,
        stepped_up,
        stepped_down,
        stepped_norm,
        stepped_bias,
        state_new_up,
        state_new_down,
        state_new_norm,
        state_new_bias,
    )


chunks = 4
pieces = 4
lanes = 128
gathered = 2


def lane_sums(x):
    total = x[:, :lanes]
    for at in range(lanes, x.shape[1], lanes):
        total = total + x[:, at : at + lanes]
    return total


def blocks(count, step):
    def over(body):
        @pl.loop(0, count // step)
        def _(at):
            body(pl.multiple_of(at * step, step))

    return over


def wait_for(ref, sem):
    pltpu.make_async_copy(ref, ref, sem).wait()


def scale_of(total, rate):
    return jnp.sqrt(total[0:1, :]) * (lax.rsqrt(total[1:2, :] * (rate * rate) + 1e-06) * rate)


def scale_at(stat, first, n, rate):
    total = stat[first]
    for at in range(1, n):
        total = total + stat[first + at]
    return scale_of(total, rate)


def exchange(
    pu, pd, pn, pb, mu_h, md_h, mn, mb, eu_h, ed_h, en, eb,
    cu, cn, cb, su, sn, sb, tu, tn, tb,
    sum_d, base_d, ed, give_d, other_d, stat_d,
    own_u, own_d, give_u, sum_u, base_u, other_u, mu, md, eu,
    pn_v, pb_v, mn_v, mb_v, en_v, eb_v, vec, got_vec,
    sq_u, sq_o, acc_d, stat_u, stat_w,
    load_sem, small_sem, part_sem, send_sem, stat_sem, more_sem, hello, ready,
):
    me = lax.axis_index("dp")
    peer = 1 - me
    here = lax.axis_index("tp")
    n = lax.axis_size("tp")
    rate = lax.axis_size("dp") ** (-0.5)
    rows, wide = mu.shape
    tall, cols = md.shape
    groups = rows // lanes
    part_d = tall // chunks
    step_u, step_d = 32, 64
    first = gathered * lanes
    rest = pl.ds(first, rows - first)

    def at_core(core, size, start=0, count=None):
        return pl.ds(pl.multiple_of(core * size + start, 8), size if count is None else count)

    def columns(core):
        return pl.ds(pl.multiple_of(core * cols, cols), cols)

    def load(source, target, sem):
        copy = pltpu.make_async_copy(source, target, sem)
        copy.start()
        return copy

    small = [
        load(source, target, small_sem.at[at])
        for at, (source, target) in enumerate(
            ((pn, pn_v), (pb, pb_v), (mn, mn_v), (mb, mb_v), (en, en_v), (eb, eb_v))
        )
    ]
    load(pu.at[at_core(me, rows), :], own_u, load_sem.at[1])
    load(mu_h, mu, load_sem.at[0])

    barrier = pltpu.get_barrier_semaphore()

    @pl.when(me == 1)
    def _():
        pl.semaphore_signal(barrier, inc=1, device_id={"dp": peer})

    @pl.when(me == 0)
    def _():
        pl.semaphore_wait(barrier, 1)
        pl.semaphore_signal(hello, inc=1, device_id={"dp": peer})

    @pl.when(me == 1)
    def _():
        pl.semaphore_wait(hello, 1)
        for step in range(1, n):
            pl.semaphore_signal(barrier, inc=1, device_id={"tp": lax.rem(here + step, n)})

    def to_peer(source, target, send, recv):
        copy = pltpu.make_async_remote_copy(
            src_ref=source, dst_ref=target, send_sem=send_sem.at[send], recv_sem=recv, device_id={"dp": peer}
        )
        copy.start()
        return copy

    spans_u = [pl.ds(at * lanes, lanes) for at in range(groups)]
    spans_d = [pl.ds(0, tall - part_d), pl.ds(tall - part_d, part_d)]
    sent = [
        to_peer(pu.at[at_core(peer, rows, at * lanes, lanes), :], sum_u.at[span, :], 0, part_sem.at[at])
        for at, span in enumerate(spans_u)
    ] + [
        to_peer(pd.at[span, columns(peer)], sum_d.at[span, :], 0, part_sem.at[groups + at])
        for at, span in enumerate(spans_d)
    ]
    load(md_h, md, load_sem.at[2])
    load(ed_h, ed, load_sem.at[3])
    load(eu_h, eu, load_sem.at[5])
    load(pd.at[:, columns(me)], own_d, load_sem.at[4])

    wait_for(mu, load_sem.at[0])

    @blocks(rows, step_u)
    def _(at):
        span = pl.ds(at, step_u)
        x = mu[span, :]
        sq_u[span, :] = lane_sums(x * x)

    def store_size(group, which):
        size = jnp.sum(sq_u[spans_u[group], :].T, axis=0).reshape(1, 1, lanes)
        if group < gathered:
            stat_u[pl.ds(group * n + here, 1), which : which + 1, :] = size
        else:
            at = (2 * (group - gathered) + me) * n + here
            stat_w[pl.ds(at, 1), which : which + 1, :] = size

    for group in range(groups):
        store_size(group, 0)

    def sizes(ref, at, send, recv, cores):
        for step in range(n):
            for core in range(cores):
                if step + core > 0:
                    pltpu.make_async_remote_copy(
                        src_ref=ref.at[at],
                        dst_ref=ref.at[at],
                        send_sem=send_sem.at[send],
                        recv_sem=recv,
                        device_id={"dp": peer if core else me, "tp": lax.rem(here + step, n)},
                    ).start()

    wait_for(own_u, load_sem.at[1])
    load(pu.at[at_core(peer, rows, first, rows - first), :], give_u, load_sem.at[6])
    load(pd.at[:, columns(peer)], give_d, load_sem.at[7])
    def sum_rows(group):
        sent[group].wait_recv()

        @blocks(lanes, step_u)
        def _(at):
            span = pl.ds(pl.multiple_of(group * lanes + at, step_u), step_u)
            x = own_u[span, :] + sum_u[span, :]
            sum_u[span, :] = x
            sq_u[span, :] = lane_sums(x * x)

        store_size(group, 1)

    def send_sizes(group):
        if group < gathered:
            sizes(stat_u, group * n + here, 1, stat_sem.at[group], 1)
        else:
            sizes(stat_w, (2 * (group - gathered) + me) * n + here, 2, stat_sem.at[group], 2)

    sum_rows(0)
    half = mn.shape[-1]
    for copy in small:
        copy.wait()
    vec[0:1, :] = pn_v[...]
    vec[1:2, :] = pb_v[...]
    vec[2:3, :half] = mn_v[...].reshape(1, half)
    vec[2:3, half:] = en_v[...].reshape(1, half)
    vec[3:4, :half] = mb_v[...].reshape(1, half)
    vec[3:4, half:] = eb_v[...].reshape(1, half)
    send_vec = to_peer(vec, got_vec, 6, more_sem.at[2])

    wait_for(md, load_sem.at[2])
    wait_for(ed, load_sem.at[3])
    acc_d[...] = jnp.zeros_like(acc_d)

    def eighths(x):
        return jnp.sum(x.reshape(step_d // 8, 8, cols), axis=0)

    @blocks(tall, step_d)
    def _(at):
        span = pl.ds(at, step_d)
        x = md[span, :]
        base_d[span, :] = x - (learn_rate * hold_rate) * ed[span, :]
        acc_d[...] += eighths(x * x)

    slot_d = me * n + here
    stat_d[pl.ds(slot_d, 1), 0:1, :] = jnp.sum(acc_d[...], axis=0).reshape(1, 1, cols)
    acc_d[...] = jnp.zeros_like(acc_d)
    wait_for(eu, load_sem.at[5])

    @blocks(rows - first, step_u)
    def _(at):
        span = pl.ds(pl.multiple_of(first + at, step_u), step_u)
        base_u[pl.ds(at, step_u), :] = mu[span, :] - (learn_rate * hold_rate) * eu[span, :]

    wait_for(own_d, load_sem.at[4])
    to_peer(own_u.at[rest, :], other_u.at[0], 3, more_sem.at[0])
    to_peer(base_u, other_u.at[1], 3, more_sem.at[0])
    to_peer(own_d, other_d.at[0], 4, more_sem.at[1])
    to_peer(base_d, other_d.at[1], 4, more_sem.at[1])

    for group in range(1, groups - 1):
        sum_rows(group)
    @pl.when(me == 1)
    def _():
        pl.semaphore_wait(barrier, n - 1)
        pl.semaphore_signal(ready, inc=1, device_id={"dp": peer})

    @pl.when(me == 0)
    def _():
        pl.semaphore_wait(ready, 1)

    for group in range(groups - 1):
        send_sizes(group)
    sum_rows(groups - 1)
    send_sizes(groups - 1)

    for chunk, part in enumerate(spans_d):
        sent[groups + chunk].wait_recv()

        @blocks(part.size, step_d)
        def _(at):
            span = pl.ds(pl.multiple_of(part.start + at, step_d), step_d)
            x = own_d[span, :] + sum_d[span, :]
            sum_d[span, :] = x
            acc_d[...] += eighths(x * x)

    stat_d[pl.ds(slot_d, 1), 1:2, :] = jnp.sum(acc_d[...], axis=0).reshape(1, 1, cols)
    sizes(stat_d, slot_d, 5, stat_sem.at[groups], 2)

    for group in range(groups):
        span = spans_u[group]
        if group < gathered:
            wait_for(stat_u.at[pl.ds(0, n - 1)], stat_sem.at[group])
            sq_u[span, :] = jnp.broadcast_to(scale_at(stat_u, group * n, n, rate), (lanes, lanes)).T
        else:
            wait_for(stat_w.at[pl.ds(0, 2 * n - 1)], stat_sem.at[group])
            at = 2 * (group - gathered)
            sq_u[span, :] = jnp.broadcast_to(scale_at(stat_w, (at + me) * n, n, rate), (lanes, lanes)).T
            sq_o[pl.ds((group - gathered) * lanes, lanes), :] = jnp.broadcast_to(
                scale_at(stat_w, (at + peer) * n, n, rate), (lanes, lanes)
            ).T
        if group < gathered:

            @blocks(lanes, step_u)
            def _(at):
                start = pl.multiple_of(group * lanes + at, step_u)
                span = pl.ds(start, step_u)
                scale = jnp.concatenate([sq_u[span, :]] * (wide // lanes), axis=1)
                state = hold_rate * eu[span, :] + sum_u[span, :] * scale
                stepped = mu[span, :] - learn_rate * state
                tu[span, :] = state
                su[span, :] = stepped
                cu[pl.ds(pl.multiple_of(me * rows + start, step_u), step_u), :] = stepped.astype(cu.dtype)

            part = cu.at[at_core(me, rows, group * lanes, lanes), :]
            to_peer(part, part, 7, more_sem.at[3])
        else:
            if group == gathered:
                wait_for(other_u, more_sem.at[0])
                wait_for(give_u, load_sem.at[6])

            @blocks(lanes, step_u // 2)
            def _(at):
                inner = pl.multiple_of((group - gathered) * lanes + at, step_u // 2)
                start = pl.multiple_of(group * lanes + at, step_u // 2)
                near, span = pl.ds(inner, step_u // 2), pl.ds(start, step_u // 2)
                scale = jnp.concatenate([sq_u[span, :]] * (wide // lanes), axis=1)
                step = sum_u[span, :] * scale
                tu[span, :] = hold_rate * eu[span, :] + step
                stepped = base_u[near, :] - learn_rate * step
                su[span, :] = stepped
                place = pl.ds(pl.multiple_of(me * rows + start, step_u // 2), step_u // 2)
                cu[place, :] = stepped.astype(cu.dtype)
                scale = jnp.concatenate([sq_o[near, :]] * (wide // lanes), axis=1)
                step = (give_u[near, :] + other_u[0, near, :]) * scale
                stepped = other_u[1, near, :] - learn_rate * step
                place = pl.ds(pl.multiple_of(peer * rows + start, step_u // 2), step_u // 2)
                cu[place, :] = stepped.astype(cu.dtype)

    send_vec.wait_recv()
    mean = (vec[0:2, :] + got_vec[0:2, :]) * rate
    for at, (state, stepped, rounded) in enumerate(((tn, sn, cn), (tb, sb, cb))):
        row = slice(2 + at, 3 + at)
        low, high = mean[at : at + 1, :half], mean[at : at + 1, half:]
        new_own = hold_rate * vec[row, half:] + jnp.where(me == 0, low, high)
        own = vec[row, :half] - learn_rate * new_own
        new_other = hold_rate * got_vec[row, half:] + jnp.where(me == 0, high, low)
        other = got_vec[row, :half] - learn_rate * new_other
        state[...] = new_own.reshape(state.shape)
        stepped[...] = own.reshape(stepped.shape)
        whole = jnp.concatenate(
            [jnp.where(me == 0, own, other), jnp.where(me == 0, other, own)], axis=1
        )
        rounded[...] = whole.reshape(rounded.shape).astype(rounded.dtype)

    wait_for(give_d, load_sem.at[7])
    wait_for(other_d, more_sem.at[1])
    wait_for(other_d, send_sem.at[0])
    wait_for(other_u, send_sem.at[3])
    wait_for(other_d, send_sem.at[4])
    send_vec.wait_send()
    wait_for(stat_u.at[pl.ds(0, gathered * (n - 1))], send_sem.at[1])
    wait_for(stat_w.at[pl.ds(0, (groups - gathered) * (2 * n - 1))], send_sem.at[2])
    wait_for(stat_d.at[pl.ds(0, 2 * n - 1)], stat_sem.at[groups])
    wait_for(stat_d.at[pl.ds(0, 2 * n - 1)], send_sem.at[5])
    wait_for(cu.at[at_core(peer, rows, 0, first), :], more_sem.at[3])
    wait_for(cu.at[at_core(me, rows, 0, first), :], send_sem.at[7])


def finish(
    cu_v, cn_v, cb_v, su_v, sn_v, sb_v, tu_v, tn_v, tb_v,
    sum_d, base_d, ed, give_d, other_d, stat_d,
    cu, cd, cn, cb, su, sd, sn, sb, tu, td, tn, tb,
    cd_v, sd_v, td_v, sem,
):
    me = lax.axis_index("dp")
    rate = lax.axis_size("dp") ** (-0.5)
    n = lax.axis_size("tp")
    tall, cols = td_v.shape
    step = 32

    def out(source, target, at):
        copy = pltpu.make_async_copy(source, target, sem.at[at])
        copy.start()
        return copy

    small = [
        out(source, target, 4 + at)
        for at, (source, target) in enumerate(
            ((cn_v, cn), (cb_v, cb), (sn_v, sn), (sb_v, sb), (tn_v, tn), (tb_v, tb))
        )
    ]
    out(su_v, su, 0)
    out(tu_v, tu, 0)
    out(cu_v, cu, 1)

    own, other = (scale_at(stat_d, core * n, n, rate) for core in (me, 1 - me))
    for piece in range(pieces):
        size = tall // pieces

        @blocks(size, step)
        def _(at):
            span = pl.ds(pl.multiple_of(piece * size + at, step), step)
            x = sum_d[span, :] * own
            td_v[span, :] = hold_rate * ed[span, :] + x
            stepped = base_d[span, :] - learn_rate * x
            sd_v[span, :] = stepped
            cd_v[span, pl.ds(pl.multiple_of(me * cols, cols), cols)] = stepped.astype(cd_v.dtype)
            x = (give_d[span, :] + other_d[0, span, :]) * other
            stepped = other_d[1, span, :] - learn_rate * x
            cd_v[span, pl.ds(pl.multiple_of((1 - me) * cols, cols), cols)] = stepped.astype(cd_v.dtype)

        span = pl.ds(piece * size, size)
        out(td_v.at[span, :], td.at[span, :], 2)
        out(sd_v.at[span, :], sd.at[span, :], 2)
        out(cd_v.at[span, :], cd.at[span, :], 3)
    for copy in small:
        copy.wait()
    wait_for(other_d, sem.at[0])
    wait_for(cu_v, sem.at[1])
    wait_for(other_d, sem.at[2])
    wait_for(cd_v, sem.at[3])


def held(arrays):
    return [pltpu.with_memory_space_constraint(x, pltpu.HBM) for x in arrays]


def on_pair(*args):
    pu, pd, pn, pb, mu, md, mn, mb, eu, ed, en, eb = args
    n = lax.axis_size("tp")
    f32, bf16 = jnp.float32, jnp.bfloat16
    vmem = pl.BlockSpec(memory_space=pltpu.VMEM)
    hbm = pl.BlockSpec(memory_space=pltpu.HBM)
    wide, tall = pu.shape[2], pd.shape[1]
    rows, cols = mu.shape[0], md.shape[1]
    groups = rows // lanes
    rest = rows - gathered * lanes
    dma = pltpu.SemaphoreType.DMA

    def shaped(shape, dtype=f32):
        return jax.ShapeDtypeStruct(shape, dtype)

    between = [
        shaped((pu.shape[1], wide), bf16), shaped((pn.shape[1],), bf16), shaped((pb.shape[1],), bf16),
        *(shaped(x.shape) for x in (mu, mn, mb)),
        *(shaped(x.shape) for x in (mu, mn, mb)),
        *(shaped(md.shape) for _ in range(4)),
        shaped((2, *md.shape)),
        shaped((2 * n, 2, cols)),
    ]
    results = pl.pallas_call(
        exchange,
        out_shape=between,
        in_specs=[hbm] * len(args),
        out_specs=[vmem] * len(between),
        scratch_shapes=[
            pltpu.VMEM(mu.shape, f32),
            pltpu.VMEM(md.shape, f32),
            pltpu.VMEM((rest, wide), f32),
            pltpu.VMEM(mu.shape, f32),
            pltpu.VMEM((rest, wide), f32),
            pltpu.VMEM((2, rest, wide), f32),
            *(pltpu.VMEM(x.shape, f32) for x in (mu, md, mu)),
            *(pltpu.VMEM(x.shape, f32) for x in (pn, pb, mn, mb, en, eb)),
            pltpu.VMEM((4, pn.shape[1]), f32),
            pltpu.VMEM((4, pn.shape[1]), f32),
            pltpu.VMEM((rows, lanes), f32),
            pltpu.VMEM((rest, lanes), f32),
            pltpu.VMEM((8, cols), f32),
            pltpu.VMEM((gathered * n, 2, lanes), f32),
            pltpu.VMEM(((groups - gathered) * 2 * n, 2, lanes), f32),
            dma((8,)),
            dma((6,)),
            dma((groups + 2,)),
            dma((8,)),
            dma((groups + 1,)),
            dma((4,)),
            pltpu.SemaphoreType.REGULAR,
            pltpu.SemaphoreType.REGULAR,
        ],
        compiler_params=pltpu.CompilerParams(
            collective_id=0, has_side_effects=True, vmem_limit_bytes=40 * 2**20
        ),
        name="exchange",
    )(*held((pu[0], pd[0], *args[2:])))
    outs = (
        ((pu.shape[1], wide), bf16),
        ((tall, pd.shape[2]), bf16),
        ((pn.shape[1],), bf16),
        ((pb.shape[1],), bf16),
        *((x.shape, f32) for x in (mu, md, mn, mb)),
        *((x.shape, f32) for x in (mu, md, mn, mb)),
    )
    return tuple(pl.pallas_call(
        finish,
        out_shape=[shaped(shape, dtype) for shape, dtype in outs],
        in_specs=[vmem] * len(between),
        out_specs=[hbm] * len(outs),
        scratch_shapes=[
            pltpu.VMEM((tall, pd.shape[2]), bf16),
            pltpu.VMEM(md.shape, f32),
            pltpu.VMEM(md.shape, f32),
            dma((10,)),
        ],
        compiler_params=pltpu.CompilerParams(vmem_limit_bytes=8 * 2**20),
        name="finish",
    )(*results))


def solution(mesh):
    in_specs = (
        P(("job", "dp"), None, "tp"),
        P(("job", "dp"), "tp", None),
        P(("job", "dp"), None),
        P(("job", "dp"), None),
        P(("job", "dp"), "tp"),
        P(("job", "tp"), "dp"),
        P(("job", "dp")),
        P(("job", "dp")),
        P(("job", "dp"), "tp"),
        P(("job", "tp"), "dp"),
        P(("job", "dp")),
        P(("job", "dp")),
    )
    out_specs = (
        P("job", "tp"),
        P(("job", "tp"), None),
        P("job"),
        P("job"),
        P(("job", "dp"), "tp"),
        P(("job", "tp"), "dp"),
        P(("job", "dp")),
        P(("job", "dp")),
        P(("job", "dp"), "tp"),
        P(("job", "tp"), "dp"),
        P(("job", "dp")),
        P(("job", "dp")),
    )
    return jax.shard_map(
        on_device if mesh.shape["dp"] != 2 else on_pair, mesh=mesh, in_specs=in_specs, out_specs=out_specs, check_vma=False
    )
```

```python
import functools

import jax
import jax.numpy as jnp
from jax import lax
from jax.experimental import pallas as pl
from jax.experimental.pallas import tpu as pltpu
from jax.sharding import PartitionSpec as P

learn_rate = 0.4
hold_rate = 0.9


def on_device(
    partial_up,
    partial_down,
    partial_norm,
    partial_bias,
    master_up,
    master_down,
    master_norm,
    master_bias,
    memory_up,
    memory_down,
    memory_norm,
    memory_bias,
):
    mean_up, mean_down = (
        lax.psum_scatter(partial_up[0], "dp", scatter_dimension=0, tiled=True),
        lax.psum_scatter(partial_down[0], "dp", scatter_dimension=1, tiled=True),
    )
    whole_norm, whole_bias = lax.psum((partial_norm[0], partial_bias[0]), "dp")
    place = lax.axis_index("dp")
    mean_norm = lax.dynamic_slice_in_dim(
        whole_norm, place * master_norm.shape[0], master_norm.shape[0]
    )
    mean_bias = lax.dynamic_slice_in_dim(
        whole_bias, place * master_bias.shape[0], master_bias.shape[0]
    )
    mean_rate = lax.axis_size("dp") ** (-0.5)
    mean_up = mean_up * mean_rate
    mean_down = mean_down * mean_rate
    mean_norm = mean_norm * mean_rate
    mean_bias = mean_bias * mean_rate
    own_up, own_down, slope_up_norm, slope_down_norm = lax.psum(
        (
            jnp.sum(master_up * master_up, axis=1, keepdims=True),
            jnp.sum(master_down * master_down, axis=0, keepdims=True),
            jnp.sum(mean_up * mean_up, axis=1, keepdims=True),
            jnp.sum(mean_down * mean_down, axis=0, keepdims=True),
        ),
        "tp",
    )
    mean_up = mean_up * (jnp.sqrt(own_up) * lax.rsqrt(slope_up_norm + 1e-06))
    mean_down = mean_down * (jnp.sqrt(own_down) * lax.rsqrt(slope_down_norm + 1e-06))
    state_new_up = hold_rate * memory_up + mean_up
    stepped_up = master_up - learn_rate * state_new_up
    state_new_down = hold_rate * memory_down + mean_down
    stepped_down = master_down - learn_rate * state_new_down
    state_new_norm = hold_rate * memory_norm + mean_norm
    stepped_norm = master_norm - learn_rate * state_new_norm
    state_new_bias = hold_rate * memory_bias + mean_bias
    stepped_bias = master_bias - learn_rate * state_new_bias
    compute_up, compute_down, compute_norm, compute_bias = (
        lax.all_gather(stepped_up.astype(jnp.bfloat16), "dp", axis=0, tiled=True),
        lax.all_gather(stepped_down.astype(jnp.bfloat16), "dp", axis=1, tiled=True),
        lax.all_gather(stepped_norm.astype(jnp.bfloat16), "dp", axis=0, tiled=True),
        lax.all_gather(stepped_bias.astype(jnp.bfloat16), "dp", axis=0, tiled=True),
    )
    return (
        compute_up,
        compute_down,
        compute_norm,
        compute_bias,
        stepped_up,
        stepped_down,
        stepped_norm,
        stepped_bias,
        state_new_up,
        state_new_down,
        state_new_norm,
        state_new_bias,
    )


pieces = 4
lanes = 128
gathered = 2


def lane_sums(x):
    total = x[:, :lanes]
    for at in range(lanes, x.shape[1], lanes):
        total = total + x[:, at : at + lanes]
    return total


def blocks(count, step):
    def over(body):
        @pl.loop(0, count // step)
        def _(at):
            body(pl.multiple_of(at * step, step))

    return over


def wait_for(ref, sem):
    pltpu.make_async_copy(ref, ref, sem).wait()


def scale_of(weights, sizes, rate):
    return jnp.sqrt(weights) * (lax.rsqrt(sizes * (rate * rate) + 1e-06) * rate)


def scale_at(stat, first, n, rate):
    total = stat[first]
    for at in range(1, n):
        total = total + stat[first + at]
    return scale_of(total[0:1, :], total[1:2, :], rate)


def exchange(
    pu, pd, pn, pb, mu_h, md_h, mn, mb, eu_h, ed_h, en, eb,
    cu, cn, cb, su, sn, sb, tu, tn, tb,
    pack, ed, stat_d,
    own_u, own_d, give_u, sum_u, base_u, other_u, mu, md, eu,
    pn_v, pb_v, mn_v, mb_v, en_v, eb_v, vec, got_vec,
    sq_u, sq_o, acc_d, acc_o, stat_u, stat_w,
    load_sem, small_sem, part_sem, send_sem, stat_sem, more_sem, hello, ready,
):
    me = lax.axis_index("dp")
    peer = 1 - me
    here = lax.axis_index("tp")
    n = lax.axis_size("tp")
    rate = lax.axis_size("dp") ** (-0.5)
    rows, wide = mu.shape
    tall, cols = md.shape
    groups = rows // lanes
    step_u, step_d = 32, 64
    shared = tall // 6 // step_d * step_d
    other_d, (sum_d, base_d, give_d) = pack.at[pl.ds(0, 2)], (pack.at[at] for at in range(2, 5))
    first = gathered * lanes
    rest = pl.ds(first, rows - first)

    def at_core(core, size, start=0, count=None):
        return pl.ds(pl.multiple_of(core * size + start, 8), size if count is None else count)

    def columns(core):
        return pl.ds(pl.multiple_of(core * cols, cols), cols)

    def load(source, target, sem):
        copy = pltpu.make_async_copy(source, target, sem)
        copy.start()
        return copy

    small = [
        load(source, target, small_sem.at[at])
        for at, (source, target) in enumerate(
            ((pn, pn_v), (pb, pb_v), (mn, mn_v), (mb, mb_v), (en, en_v), (eb, eb_v))
        )
    ]
    load(pu.at[at_core(me, rows), :], own_u, load_sem.at[0])
    load(mu_h, mu, load_sem.at[0])

    barrier = pltpu.get_barrier_semaphore()

    @pl.when(me == 1)
    def _():
        pl.semaphore_signal(barrier, inc=1, device_id={"dp": peer})

    @pl.when(me == 0)
    def _():
        pl.semaphore_wait(barrier, 1)
        pl.semaphore_signal(hello, inc=1, device_id={"dp": peer})

    @pl.when(me == 1)
    def _():
        pl.semaphore_wait(hello, 1)
        for step in range(1, n):
            pl.semaphore_signal(barrier, inc=1, device_id={"tp": lax.rem(here + step, n)})

    def to_peer(source, target, send, recv):
        copy = pltpu.make_async_remote_copy(
            src_ref=source, dst_ref=target, send_sem=send, recv_sem=recv, device_id={"dp": peer}
        )
        copy.start()
        return copy

    spans_u = [pl.ds(at * lanes, lanes) for at in range(groups)]
    head, last = pl.ds(0, tall - shared), pl.ds(tall - shared, shared)
    heads = pl.ds(0, tall - 2 * shared), pl.ds(tall - 2 * shared, shared)
    sent = [
        to_peer(pu.at[at_core(peer, rows, at * lanes, lanes), :], sum_u.at[span, :], send_sem.at[0], part_sem.at[at])
        for at, span in enumerate(spans_u)
    ]
    for at, span in enumerate(heads):
        sent.append(to_peer(pd.at[span, columns(peer)], sum_d.at[span, :], send_sem.at[0], part_sem.at[groups + at]))

    @pl.when(me == 0)
    def _():
        to_peer(pd.at[last, columns(peer)], sum_d.at[last, :], send_sem.at[0], part_sem.at[groups + 2])
        to_peer(pd.at[last, columns(me)], other_d.at[0, last, :], send_sem.at[0], part_sem.at[groups + 3])

    load(md_h, md, load_sem.at[1])
    load(ed_h, ed, load_sem.at[1])
    load(eu_h, eu, load_sem.at[2])
    load(pd.at[:, columns(me)], own_d, load_sem.at[2])

    wait_for(other_d, load_sem.at[0])
    load(pd.at[:, columns(peer)], give_d, load_sem.at[0])
    for copy in small:
        copy.wait()
    load(pu.at[at_core(peer, rows, first, rows - first), :], give_u, small_sem.at[0])

    @blocks(rows, step_u)
    def _(at):
        span = pl.ds(at, step_u)
        x = mu[span, :]
        sq_u[span, :] = lane_sums(x * x)

    def store_size(group, which):
        size = jnp.sum(sq_u[spans_u[group], :].T, axis=0).reshape(1, 1, lanes)
        if group < gathered:
            stat_u[pl.ds(group * n + here, 1), which : which + 1, :] = size
        else:
            at = (2 * (group - gathered) + me) * n + here
            stat_w[pl.ds(at, 1), which : which + 1, :] = size

    for group in range(groups):
        store_size(group, 0)

    def sizes(ref, at, send, recv, cores):
        for step in range(n):
            for core in range(cores):
                if step + core > 0:
                    pltpu.make_async_remote_copy(
                        src_ref=ref.at[at],
                        dst_ref=ref.at[at],
                        send_sem=small_sem.at[send],
                        recv_sem=recv,
                        device_id={"dp": peer if core else me, "tp": lax.rem(here + step, n)},
                    ).start()

    def sum_rows(group):
        sent[group].wait_recv()

        @blocks(lanes, step_u)
        def _(at):
            span = pl.ds(pl.multiple_of(group * lanes + at, step_u), step_u)
            x = own_u[span, :] + sum_u[span, :]
            sum_u[span, :] = x
            sq_u[span, :] = lane_sums(x * x)

        store_size(group, 1)

    def send_sizes(group):
        if group < gathered:
            sizes(stat_u, group * n + here, 1, stat_sem.at[group], 1)
        else:
            sizes(stat_w, (2 * (group - gathered) + me) * n + here, 2, stat_sem.at[group], 2)

    def meet():
        @pl.when(me == 1)
        def _():
            pl.semaphore_wait(barrier, n - 1)
            pl.semaphore_signal(ready, inc=1, device_id={"dp": peer})

        @pl.when(me == 0)
        def _():
            pl.semaphore_wait(ready, 1)

    for group in range(groups - 1):
        sum_rows(group)

        @pl.when(2 * here >= n)
        def _(group=group):
            if group == 0:
                meet()
            send_sizes(group)

    half = mn.shape[-1]
    vec[0:1, :] = pn_v[...]
    vec[1:2, :] = pb_v[...]
    vec[2:3, :half] = mn_v[...].reshape(1, half)
    vec[2:3, half:] = en_v[...].reshape(1, half)
    vec[3:4, :half] = mb_v[...].reshape(1, half)
    vec[3:4, half:] = eb_v[...].reshape(1, half)
    send_vec = to_peer(vec, got_vec, small_sem.at[4], more_sem.at[2])

    wait_for(other_d, load_sem.at[1])
    acc_d[...] = jnp.zeros_like(acc_d)
    acc_o[...] = jnp.zeros_like(acc_o)

    def eighths(x):
        return jnp.sum(x.reshape(step_d // 8, 8, cols), axis=0)

    @blocks(tall, step_d)
    def _(at):
        span = pl.ds(at, step_d)
        x = md[span, :]
        base_d[span, :] = x - (learn_rate * hold_rate) * ed[span, :]
        acc_d[...] += eighths(x * x)

    slot_d = me * n + here
    stat_d[pl.ds(slot_d, 1), :, :] = jnp.broadcast_to(jnp.sum(acc_d[...], axis=0).reshape(1, 1, cols), (1, 4, cols))
    acc_d[...] = jnp.zeros_like(acc_d)
    wait_for(other_d, load_sem.at[2])

    @blocks(rows - first, step_u)
    def _(at):
        span = pl.ds(pl.multiple_of(first + at, step_u), step_u)
        base_u[pl.ds(at, step_u), :] = mu[span, :] - (learn_rate * hold_rate) * eu[span, :]

    to_peer(own_u.at[rest, :], other_u.at[0], send_sem.at[0], more_sem.at[0])
    to_peer(base_u, other_u.at[1], send_sem.at[0], more_sem.at[0])

    @pl.when(me == 0)
    def _():
        to_peer(own_d.at[head, :], other_d.at[0, head, :], send_sem.at[0], more_sem.at[1])

    @pl.when(me == 1)
    def _():
        to_peer(own_d, other_d.at[0], send_sem.at[0], more_sem.at[1])
        to_peer(pd.at[last, columns(peer)], sum_d.at[last, :], send_sem.at[0], part_sem.at[groups + 2])

    to_peer(base_d, other_d.at[1], send_sem.at[0], more_sem.at[4])

    @pl.when(2 * here < n)
    def _():
        meet()
        for group in range(groups - 1):
            send_sizes(group)

    sum_rows(groups - 1)
    send_sizes(groups - 1)

    def sum_columns(part, acc, one, two, total=None):
        @blocks(part.size, step_d)
        def _(at):
            span = pl.ds(pl.multiple_of(part.start + at, step_d), step_d)
            x = one[span, :] + two[span, :]
            if total is not None:
                total[span, :] = x
            if acc is not None:
                acc[...] += eighths(x * x)

    wait_for(give_d, load_sem.at[0])
    for at, span in enumerate(heads):
        sent[groups + at].wait_recv()
        sum_columns(span, acc_d, own_d, sum_d, sum_d)

    @pl.when(me == 1)
    def _():
        wait_for(sum_d.at[last, :], part_sem.at[groups + 2])
        sum_columns(last, acc_d, own_d, sum_d, sum_d)
        wait_for(sum_d.at[last, :], part_sem.at[groups + 3])
        sum_columns(last, acc_o, give_d, other_d.at[0])

    stat_d[pl.ds(slot_d, 1), 1:2, :] = jnp.sum(acc_d[...], axis=0).reshape(1, 1, cols)
    stat_d[pl.ds(slot_d, 1), 2:3, :] = jnp.sum(acc_o[...], axis=0).reshape(1, 1, cols)
    sizes(stat_d, slot_d, 3, stat_sem.at[groups], 2)

    for group in range(groups):
        span = spans_u[group]
        if group < gathered:
            wait_for(stat_u.at[pl.ds(0, n - 1)], stat_sem.at[group])
            sq_u[span, :] = jnp.broadcast_to(scale_at(stat_u, group * n, n, rate), (lanes, lanes)).T
        else:
            wait_for(stat_w.at[pl.ds(0, 2 * n - 1)], stat_sem.at[group])
            at = 2 * (group - gathered)
            sq_u[span, :] = jnp.broadcast_to(scale_at(stat_w, (at + me) * n, n, rate), (lanes, lanes)).T
            sq_o[pl.ds((group - gathered) * lanes, lanes), :] = jnp.broadcast_to(
                scale_at(stat_w, (at + peer) * n, n, rate), (lanes, lanes)
            ).T
        if group < gathered:

            @blocks(lanes, step_u)
            def _(at):
                start = pl.multiple_of(group * lanes + at, step_u)
                span = pl.ds(start, step_u)
                scale = jnp.concatenate([sq_u[span, :]] * (wide // lanes), axis=1)
                state = hold_rate * eu[span, :] + sum_u[span, :] * scale
                stepped = mu[span, :] - learn_rate * state
                tu[span, :] = state
                su[span, :] = stepped
                cu[pl.ds(pl.multiple_of(me * rows + start, step_u), step_u), :] = stepped.astype(cu.dtype)

            part = cu.at[at_core(me, rows, group * lanes, lanes), :]
            to_peer(part, part, send_sem.at[0], more_sem.at[3])
        else:
            if group == gathered:
                wait_for(other_u, more_sem.at[0])
                wait_for(give_u, small_sem.at[0])

            @blocks(lanes, step_u // 2)
            def _(at):
                inner = pl.multiple_of((group - gathered) * lanes + at, step_u // 2)
                start = pl.multiple_of(group * lanes + at, step_u // 2)
                near, span = pl.ds(inner, step_u // 2), pl.ds(start, step_u // 2)
                scale = jnp.concatenate([sq_u[span, :]] * (wide // lanes), axis=1)
                step = sum_u[span, :] * scale
                tu[span, :] = hold_rate * eu[span, :] + step
                stepped = base_u[near, :] - learn_rate * step
                su[span, :] = stepped
                place = pl.ds(pl.multiple_of(me * rows + start, step_u // 2), step_u // 2)
                cu[place, :] = stepped.astype(cu.dtype)
                scale = jnp.concatenate([sq_o[near, :]] * (wide // lanes), axis=1)
                step = (give_u[near, :] + other_u[0, near, :]) * scale
                stepped = other_u[1, near, :] - learn_rate * step
                place = pl.ds(pl.multiple_of(peer * rows + start, step_u // 2), step_u // 2)
                cu[place, :] = stepped.astype(cu.dtype)

    send_vec.wait_recv()
    mean = (vec[0:2, :] + got_vec[0:2, :]) * rate
    for at, (state, stepped, rounded) in enumerate(((tn, sn, cn), (tb, sb, cb))):
        row = slice(2 + at, 3 + at)
        low, high = mean[at : at + 1, :half], mean[at : at + 1, half:]
        new_own = hold_rate * vec[row, half:] + jnp.where(me == 0, low, high)
        own = vec[row, :half] - learn_rate * new_own
        new_other = hold_rate * got_vec[row, half:] + jnp.where(me == 0, high, low)
        other = got_vec[row, :half] - learn_rate * new_other
        state[...] = new_own.reshape(state.shape)
        stepped[...] = own.reshape(stepped.shape)
        whole = jnp.concatenate(
            [jnp.where(me == 0, own, other), jnp.where(me == 0, other, own)], axis=1
        )
        rounded[...] = whole.reshape(rounded.shape).astype(rounded.dtype)

    @pl.when(me == 0)
    def _():
        wait_for(sum_d.at[last, :], part_sem.at[groups + 2])
        sum_columns(last, None, own_d, sum_d, sum_d)
        wait_for(pack.at[0], more_sem.at[1])

    @pl.when(me == 1)
    def _():
        wait_for(pack.at[0, head, :], more_sem.at[1])

    wait_for(base_d, more_sem.at[4])

    send_vec.wait_send()
    wait_for(stat_u.at[pl.ds(0, gathered * (n - 1))], small_sem.at[1])
    wait_for(stat_w.at[pl.ds(0, (groups - gathered) * (2 * n - 1))], small_sem.at[2])
    wait_for(stat_d.at[pl.ds(0, 2 * n - 1)], stat_sem.at[groups])
    wait_for(stat_d.at[pl.ds(0, 2 * n - 1)], small_sem.at[3])
    wait_for(cu.at[at_core(peer, rows, 0, first), :], more_sem.at[3])
    wait_for(pack, send_sem.at[0])


def finish(
    cu_v, cn_v, cb_v, su_v, sn_v, sb_v, tu_v, tn_v, tb_v,
    pack, ed, stat_d,
    cu, cd, cn, cb, su, sd, sn, sb, tu, td, tn, tb,
    cd_v, sd_v, td_v, sem,
):
    me = lax.axis_index("dp")
    rate = lax.axis_size("dp") ** (-0.5)
    n = lax.axis_size("tp")
    tall, cols = td_v.shape
    step = 32
    mine_d, base_o, sum_d, base_d, give_d = (pack.at[at] for at in range(5))

    def out(source, target, at):
        copy = pltpu.make_async_copy(source, target, sem.at[at])
        copy.start()
        return copy

    small = [
        out(source, target, 2 + at)
        for at, (source, target) in enumerate(
            ((cn_v, cn), (cb_v, cb), (sn_v, sn), (sb_v, sb), (tn_v, tn), (tb_v, tb))
        )
    ]
    out(su_v, su, 0)
    out(tu_v, tu, 0)
    out(cu_v, cu, 1)

    scales = []
    for core in (me, 1 - me):
        weights = sizes = 0.0
        for at in range(n):
            near, far = stat_d[core * n + at], stat_d[(1 - core) * n + at]
            weights = weights + near[0:1, :]
            sizes = sizes + near[1:2, :] + far[2:3, :]
        scales.append(scale_of(weights, sizes, rate))
    own, other = scales
    for piece in range(pieces):
        size = tall // pieces

        @blocks(size, step)
        def _(at):
            span = pl.ds(pl.multiple_of(piece * size + at, step), step)
            x = sum_d[span, :] * own
            td_v[span, :] = hold_rate * ed[span, :] + x
            stepped = base_d[span, :] - learn_rate * x
            sd_v[span, :] = stepped
            cd_v[span, pl.ds(pl.multiple_of(me * cols, cols), cols)] = stepped.astype(cd_v.dtype)
            x = (give_d[span, :] + mine_d[span, :]) * other
            stepped = base_o[span, :] - learn_rate * x
            cd_v[span, pl.ds(pl.multiple_of((1 - me) * cols, cols), cols)] = stepped.astype(cd_v.dtype)

        span = pl.ds(piece * size, size)
        out(td_v.at[span, :], td.at[span, :], 0)
        out(sd_v.at[span, :], sd.at[span, :], 0)
        out(cd_v.at[span, :], cd.at[span, :], 0)
    for copy in small:
        copy.wait()
    wait_for(cu_v, sem.at[1])
    wait_for(pack, sem.at[0])


def held(arrays):
    return [pltpu.with_memory_space_constraint(x, pltpu.HBM) for x in arrays]


def on_pair(*args):
    pu, pd, pn, pb, mu, md, mn, mb, eu, ed, en, eb = args
    n = lax.axis_size("tp")
    f32, bf16 = jnp.float32, jnp.bfloat16
    vmem = pl.BlockSpec(memory_space=pltpu.VMEM)
    hbm = pl.BlockSpec(memory_space=pltpu.HBM)
    wide, tall = pu.shape[2], pd.shape[1]
    rows, cols = mu.shape[0], md.shape[1]
    groups = rows // lanes
    rest = rows - gathered * lanes
    dma = pltpu.SemaphoreType.DMA

    def shaped(shape, dtype=f32):
        return jax.ShapeDtypeStruct(shape, dtype)

    between = [
        shaped((pu.shape[1], wide), bf16), shaped((pn.shape[1],), bf16), shaped((pb.shape[1],), bf16),
        *(shaped(x.shape) for x in (mu, mn, mb)),
        *(shaped(x.shape) for x in (mu, mn, mb)),
        shaped((5, *md.shape)),
        shaped(md.shape),
        shaped((2 * n, 4, cols)),
    ]
    results = pl.pallas_call(
        exchange,
        out_shape=between,
        in_specs=[hbm] * len(args),
        out_specs=[vmem] * len(between),
        scratch_shapes=[
            pltpu.VMEM(mu.shape, f32),
            pltpu.VMEM(md.shape, f32),
            pltpu.VMEM((rest, wide), f32),
            pltpu.VMEM(mu.shape, f32),
            pltpu.VMEM((rest, wide), f32),
            pltpu.VMEM((2, rest, wide), f32),
            *(pltpu.VMEM(x.shape, f32) for x in (mu, md, mu)),
            *(pltpu.VMEM(x.shape, f32) for x in (pn, pb, mn, mb, en, eb)),
            pltpu.VMEM((4, pn.shape[1]), f32),
            pltpu.VMEM((4, pn.shape[1]), f32),
            pltpu.VMEM((rows, lanes), f32),
            pltpu.VMEM((rest, lanes), f32),
            pltpu.VMEM((8, cols), f32),
            pltpu.VMEM((8, cols), f32),
            pltpu.VMEM((gathered * n, 2, lanes), f32),
            pltpu.VMEM(((groups - gathered) * 2 * n, 2, lanes), f32),
            dma((3,)),
            dma((6,)),
            dma((groups + 4,)),
            dma((1,)),
            dma((groups + 1,)),
            dma((5,)),
            pltpu.SemaphoreType.REGULAR,
            pltpu.SemaphoreType.REGULAR,
        ],
        compiler_params=pltpu.CompilerParams(
            collective_id=0, has_side_effects=True, vmem_limit_bytes=40 * 2**20
        ),
        name="exchange",
    )(*held((pu[0], pd[0], *args[2:])))
    outs = (
        ((pu.shape[1], wide), bf16),
        ((tall, pd.shape[2]), bf16),
        ((pn.shape[1],), bf16),
        ((pb.shape[1],), bf16),
        *((x.shape, f32) for x in (mu, md, mn, mb)),
        *((x.shape, f32) for x in (mu, md, mn, mb)),
    )
    return tuple(pl.pallas_call(
        finish,
        out_shape=[shaped(shape, dtype) for shape, dtype in outs],
        in_specs=[vmem] * len(between),
        out_specs=[hbm] * len(outs),
        scratch_shapes=[
            pltpu.VMEM((tall, pd.shape[2]), bf16),
            pltpu.VMEM(md.shape, f32),
            pltpu.VMEM(md.shape, f32),
            dma((8,)),
        ],
        compiler_params=pltpu.CompilerParams(vmem_limit_bytes=8 * 2**20),
        name="finish",
    )(*results))


def solution(mesh):
    in_specs = (
        P(("job", "dp"), None, "tp"),
        P(("job", "dp"), "tp", None),
        P(("job", "dp"), None),
        P(("job", "dp"), None),
        P(("job", "dp"), "tp"),
        P(("job", "tp"), "dp"),
        P(("job", "dp")),
        P(("job", "dp")),
        P(("job", "dp"), "tp"),
        P(("job", "tp"), "dp"),
        P(("job", "dp")),
        P(("job", "dp")),
    )
    out_specs = (
        P("job", "tp"),
        P(("job", "tp"), None),
        P("job"),
        P("job"),
        P(("job", "dp"), "tp"),
        P(("job", "tp"), "dp"),
        P(("job", "dp")),
        P(("job", "dp")),
        P(("job", "dp"), "tp"),
        P(("job", "tp"), "dp"),
        P(("job", "dp")),
        P(("job", "dp")),
    )
    return jax.shard_map(
        on_device if mesh.shape["dp"] != 2 else on_pair, mesh=mesh, in_specs=in_specs, out_specs=out_specs, check_vma=False
    )
```

```python
import functools

import jax
import jax.numpy as jnp
from jax import lax
from jax.experimental import pallas as pl
from jax.experimental.pallas import tpu as pltpu
from jax.sharding import PartitionSpec as P

learn_rate = 0.4
hold_rate = 0.9


def on_device(
    partial_up,
    partial_down,
    partial_norm,
    partial_bias,
    master_up,
    master_down,
    master_norm,
    master_bias,
    memory_up,
    memory_down,
    memory_norm,
    memory_bias,
):
    mean_up, mean_down = (
        lax.psum_scatter(partial_up[0], "dp", scatter_dimension=0, tiled=True),
        lax.psum_scatter(partial_down[0], "dp", scatter_dimension=1, tiled=True),
    )
    whole_norm, whole_bias = lax.psum((partial_norm[0], partial_bias[0]), "dp")
    place = lax.axis_index("dp")
    mean_norm = lax.dynamic_slice_in_dim(
        whole_norm, place * master_norm.shape[0], master_norm.shape[0]
    )
    mean_bias = lax.dynamic_slice_in_dim(
        whole_bias, place * master_bias.shape[0], master_bias.shape[0]
    )
    mean_rate = lax.axis_size("dp") ** (-0.5)
    mean_up = mean_up * mean_rate
    mean_down = mean_down * mean_rate
    mean_norm = mean_norm * mean_rate
    mean_bias = mean_bias * mean_rate
    own_up, own_down, slope_up_norm, slope_down_norm = lax.psum(
        (
            jnp.sum(master_up * master_up, axis=1, keepdims=True),
            jnp.sum(master_down * master_down, axis=0, keepdims=True),
            jnp.sum(mean_up * mean_up, axis=1, keepdims=True),
            jnp.sum(mean_down * mean_down, axis=0, keepdims=True),
        ),
        "tp",
    )
    mean_up = mean_up * (jnp.sqrt(own_up) * lax.rsqrt(slope_up_norm + 1e-06))
    mean_down = mean_down * (jnp.sqrt(own_down) * lax.rsqrt(slope_down_norm + 1e-06))
    state_new_up = hold_rate * memory_up + mean_up
    stepped_up = master_up - learn_rate * state_new_up
    state_new_down = hold_rate * memory_down + mean_down
    stepped_down = master_down - learn_rate * state_new_down
    state_new_norm = hold_rate * memory_norm + mean_norm
    stepped_norm = master_norm - learn_rate * state_new_norm
    state_new_bias = hold_rate * memory_bias + mean_bias
    stepped_bias = master_bias - learn_rate * state_new_bias
    compute_up, compute_down, compute_norm, compute_bias = (
        lax.all_gather(stepped_up.astype(jnp.bfloat16), "dp", axis=0, tiled=True),
        lax.all_gather(stepped_down.astype(jnp.bfloat16), "dp", axis=1, tiled=True),
        lax.all_gather(stepped_norm.astype(jnp.bfloat16), "dp", axis=0, tiled=True),
        lax.all_gather(stepped_bias.astype(jnp.bfloat16), "dp", axis=0, tiled=True),
    )
    return (
        compute_up,
        compute_down,
        compute_norm,
        compute_bias,
        stepped_up,
        stepped_down,
        stepped_norm,
        stepped_bias,
        state_new_up,
        state_new_down,
        state_new_norm,
        state_new_bias,
    )


pieces = 4
lanes = 128
gathered = 2


def lane_sums(x):
    total = x[:, :lanes]
    for at in range(lanes, x.shape[1], lanes):
        total = total + x[:, at : at + lanes]
    return total


def blocks(count, step):
    def over(body):
        @pl.loop(0, count // step)
        def _(at):
            body(pl.multiple_of(at * step, step))

    return over


def wait_for(ref, sem):
    pltpu.make_async_copy(ref, ref, sem).wait()


def scale_of(weights, sizes, rate):
    return jnp.sqrt(weights) * (lax.rsqrt(sizes * (rate * rate) + 1e-06) * rate)


def scale_at(stat, first, n, rate):
    total = stat[first]
    for at in range(1, n):
        total = total + stat[first + at]
    return scale_of(total[0:1, :], total[1:2, :], rate)


def exchange(*refs):
    (*refs, last_sem), stat_d = refs, refs[23]
    n = stat_d.shape[0] // 2
    groups = refs[4].shape[0] // lanes
    dma, regular = pltpu.SemaphoreType.DMA, pltpu.SemaphoreType.REGULAR
    pl.run_scoped(
        functools.partial(exchange_all_but_last, *refs, last_sem),
        dma((2,)), dma((6,)), dma((groups + 4,)), dma((1,)), dma((groups,)), dma((5,)), regular, regular,
    )
    wait_for(stat_d.at[pl.ds(0, 2 * n - 1)], last_sem.at[0])


def exchange_all_but_last(
    pu, pd, pn, pb, mu_h, md_h, mn, mb, eu_h, ed_h, en, eb,
    cu, cn, cb, su, sn, sb, tu, tn, tb,
    pack, ed, stat_d,
    own_u, own_d, give_u, sum_u, base_u, other_u, mu, md, eu,
    pn_v, pb_v, mn_v, mb_v, en_v, eb_v, vec, got_vec,
    sq_u, sq_o, acc_d, acc_o, stat_u, stat_w,
    last_sem, load_sem, small_sem, part_sem, send_sem, stat_sem, more_sem, hello, ready,
):
    me = lax.axis_index("dp")
    peer = 1 - me
    here = lax.axis_index("tp")
    n = lax.axis_size("tp")
    rate = lax.axis_size("dp") ** (-0.5)
    rows, wide = mu.shape
    tall, cols = md.shape
    groups = rows // lanes
    step_u, step_d = 32, 64
    shared = tall // 6 // step_d * step_d
    other_d, (sum_d, base_d, give_d) = pack.at[pl.ds(0, 2)], (pack.at[at] for at in range(2, 5))
    first = gathered * lanes
    rest = pl.ds(first, rows - first)

    def at_core(core, size, start=0, count=None):
        return pl.ds(pl.multiple_of(core * size + start, 8), size if count is None else count)

    def columns(core):
        return pl.ds(pl.multiple_of(core * cols, cols), cols)

    def load(source, target, sem):
        copy = pltpu.make_async_copy(source, target, sem)
        copy.start()
        return copy

    small = [
        load(source, target, small_sem.at[at])
        for at, (source, target) in enumerate(
            ((pn, pn_v), (pb, pb_v), (mn, mn_v), (mb, mb_v), (en, en_v), (eb, eb_v))
        )
    ]
    load(pu.at[at_core(me, rows), :], own_u, load_sem.at[0])
    load(mu_h, mu, load_sem.at[0])

    barrier = pltpu.get_barrier_semaphore()

    @pl.when(me == 1)
    def _():
        pl.semaphore_signal(barrier, inc=1, device_id={"dp": peer})

    @pl.when(me == 0)
    def _():
        pl.semaphore_wait(barrier, 1)
        pl.semaphore_signal(hello, inc=1, device_id={"dp": peer})

    @pl.when(me == 1)
    def _():
        pl.semaphore_wait(hello, 1)
        for step in range(1, n):
            pl.semaphore_signal(barrier, inc=1, device_id={"tp": lax.rem(here + step, n)})

    def to_peer(source, target, send, recv):
        copy = pltpu.make_async_remote_copy(
            src_ref=source, dst_ref=target, send_sem=send, recv_sem=recv, device_id={"dp": peer}
        )
        copy.start()
        return copy

    spans_u = [pl.ds(at * lanes, lanes) for at in range(groups)]
    head, last = pl.ds(0, tall - shared), pl.ds(tall - shared, shared)
    heads = pl.ds(0, tall - 2 * shared), pl.ds(tall - 2 * shared, shared)
    sent = [
        to_peer(pu.at[at_core(peer, rows, at * lanes, lanes), :], sum_u.at[span, :], send_sem.at[0], part_sem.at[at])
        for at, span in enumerate(spans_u)
    ]
    for at, span in enumerate(heads):
        sent.append(to_peer(pd.at[span, columns(peer)], sum_d.at[span, :], send_sem.at[0], part_sem.at[groups + at]))

    @pl.when(me == 0)
    def _():
        to_peer(pd.at[last, columns(peer)], sum_d.at[last, :], send_sem.at[0], part_sem.at[groups + 2])
        to_peer(pd.at[last, columns(me)], other_d.at[0, last, :], send_sem.at[0], part_sem.at[groups + 3])

    load(md_h, md, load_sem.at[1])
    load(ed_h, ed, load_sem.at[1])
    load(eu_h, eu, load_sem.at[1])
    load(pd.at[:, columns(me)], own_d, load_sem.at[1])

    wait_for(other_d, load_sem.at[0])
    load(pd.at[:, columns(peer)], give_d, load_sem.at[0])
    for copy in small:
        copy.wait()
    load(pu.at[at_core(peer, rows, first, rows - first), :], give_u, small_sem.at[0])

    @blocks(rows, step_u)
    def _(at):
        span = pl.ds(at, step_u)
        x = mu[span, :]
        sq_u[span, :] = lane_sums(x * x)

    def store_size(group, which):
        size = jnp.sum(sq_u[spans_u[group], :].T, axis=0).reshape(1, 1, lanes)
        if group < gathered:
            stat_u[pl.ds(group * n + here, 1), which : which + 1, :] = size
        else:
            at = (2 * (group - gathered) + me) * n + here
            stat_w[pl.ds(at, 1), which : which + 1, :] = size

    for group in range(groups):
        store_size(group, 0)

    def sizes(ref, at, send, recv, cores):
        for step in (*range(1, n), 0):
            for core in range(cores):
                if step + core > 0:
                    target = me if cores == 1 else core if step else peer
                    pltpu.make_async_remote_copy(
                        src_ref=ref.at[at],
                        dst_ref=ref.at[at],
                        send_sem=small_sem.at[send],
                        recv_sem=recv,
                        device_id={"dp": target, "tp": lax.rem(here + step, n)},
                    ).start()

    def sum_rows(group):
        sent[group].wait_recv()

        @blocks(lanes, step_u)
        def _(at):
            span = pl.ds(pl.multiple_of(group * lanes + at, step_u), step_u)
            x = own_u[span, :] + sum_u[span, :]
            sum_u[span, :] = x
            sq_u[span, :] = lane_sums(x * x)

        store_size(group, 1)

    def send_sizes(group):
        if group < gathered:
            sizes(stat_u, group * n + here, 1, stat_sem.at[group], 1)
        else:
            sizes(stat_w, (2 * (group - gathered) + me) * n + here, 2, stat_sem.at[group], 2)

    def meet():
        @pl.when(me == 1)
        def _():
            pl.semaphore_wait(barrier, n - 1)
            pl.semaphore_signal(ready, inc=1, device_id={"dp": peer})

        @pl.when(me == 0)
        def _():
            pl.semaphore_wait(ready, 1)

    for group in range(groups - 1):
        sum_rows(group)

        @pl.when(2 * here >= n)
        def _(group=group):
            if group == 0:
                meet()
            send_sizes(group)

    half = mn.shape[-1]
    vec[0:1, :] = pn_v[...]
    vec[1:2, :] = pb_v[...]
    vec[2:3, :half] = mn_v[...].reshape(1, half)
    vec[2:3, half:] = en_v[...].reshape(1, half)
    vec[3:4, :half] = mb_v[...].reshape(1, half)
    vec[3:4, half:] = eb_v[...].reshape(1, half)
    send_vec = to_peer(vec, got_vec, small_sem.at[4], more_sem.at[2])

    wait_for(pack.at[pl.ds(0, 4)], load_sem.at[1])
    acc_d[...] = jnp.zeros_like(acc_d)
    acc_o[...] = jnp.zeros_like(acc_o)

    def eighths(x):
        return jnp.sum(x.reshape(step_d // 8, 8, cols), axis=0)

    @blocks(tall, step_d)
    def _(at):
        span = pl.ds(at, step_d)
        x = md[span, :]
        base_d[span, :] = x - (learn_rate * hold_rate) * ed[span, :]
        acc_d[...] += eighths(x * x)

    slot_d = me * n + here
    stat_d[pl.ds(slot_d, 1), :, :] = jnp.broadcast_to(jnp.sum(acc_d[...], axis=0).reshape(1, 1, cols), (1, 4, cols))
    acc_d[...] = jnp.zeros_like(acc_d)

    @blocks(rows - first, step_u)
    def _(at):
        span = pl.ds(pl.multiple_of(first + at, step_u), step_u)
        base_u[pl.ds(at, step_u), :] = mu[span, :] - (learn_rate * hold_rate) * eu[span, :]

    to_peer(own_u.at[rest, :], other_u.at[0], send_sem.at[0], more_sem.at[0])
    to_peer(base_u, other_u.at[1], send_sem.at[0], more_sem.at[0])

    @pl.when(me == 0)
    def _():
        to_peer(own_d.at[head, :], other_d.at[0, head, :], send_sem.at[0], more_sem.at[1])

    @pl.when(me == 1)
    def _():
        to_peer(own_d, other_d.at[0], send_sem.at[0], more_sem.at[1])
        to_peer(pd.at[last, columns(peer)], sum_d.at[last, :], send_sem.at[0], part_sem.at[groups + 2])

    to_peer(base_d, other_d.at[1], send_sem.at[0], more_sem.at[4])

    @pl.when(2 * here < n)
    def _():
        meet()
        for group in range(groups - 1):
            send_sizes(group)

    sum_rows(groups - 1)
    send_sizes(groups - 1)

    def sum_columns(part, acc, one, two, total=None):
        @blocks(part.size, step_d)
        def _(at):
            span = pl.ds(pl.multiple_of(part.start + at, step_d), step_d)
            x = one[span, :] + two[span, :]
            if total is not None:
                total[span, :] = x
            if acc is not None:
                acc[...] += eighths(x * x)

    wait_for(give_d, load_sem.at[0])
    for at, span in enumerate(heads):
        sent[groups + at].wait_recv()
        sum_columns(span, acc_d, own_d, sum_d, sum_d)

    @pl.when(me == 1)
    def _():
        wait_for(sum_d.at[last, :], part_sem.at[groups + 2])
        sum_columns(last, acc_d, own_d, sum_d, sum_d)
        wait_for(sum_d.at[last, :], part_sem.at[groups + 3])
        sum_columns(last, acc_o, give_d, other_d.at[0])

    stat_d[pl.ds(slot_d, 1), 1:2, :] = jnp.sum(acc_d[...], axis=0).reshape(1, 1, cols)
    stat_d[pl.ds(slot_d, 1), 2:3, :] = jnp.sum(acc_o[...], axis=0).reshape(1, 1, cols)
    sizes(stat_d, slot_d, 3, last_sem.at[0], 2)

    for group in range(groups):
        span = spans_u[group]
        if group < gathered:
            wait_for(stat_u.at[pl.ds(0, n - 1)], stat_sem.at[group])
            sq_u[span, :] = jnp.broadcast_to(scale_at(stat_u, group * n, n, rate), (lanes, lanes)).T
        else:
            wait_for(stat_w.at[pl.ds(0, 2 * n - 1)], stat_sem.at[group])
            at = 2 * (group - gathered)
            sq_u[span, :] = jnp.broadcast_to(scale_at(stat_w, (at + me) * n, n, rate), (lanes, lanes)).T
            sq_o[pl.ds((group - gathered) * lanes, lanes), :] = jnp.broadcast_to(
                scale_at(stat_w, (at + peer) * n, n, rate), (lanes, lanes)
            ).T
        if group < gathered:

            @blocks(lanes, step_u)
            def _(at):
                start = pl.multiple_of(group * lanes + at, step_u)
                span = pl.ds(start, step_u)
                scale = jnp.concatenate([sq_u[span, :]] * (wide // lanes), axis=1)
                state = hold_rate * eu[span, :] + sum_u[span, :] * scale
                stepped = mu[span, :] - learn_rate * state
                tu[span, :] = state
                su[span, :] = stepped
                cu[pl.ds(pl.multiple_of(me * rows + start, step_u), step_u), :] = stepped.astype(cu.dtype)

            part = cu.at[at_core(me, rows, group * lanes, lanes), :]
            to_peer(part, part, send_sem.at[0], more_sem.at[3])
        else:
            if group == gathered:
                wait_for(other_u, more_sem.at[0])
                wait_for(give_u, small_sem.at[0])

            @blocks(lanes, step_u // 2)
            def _(at):
                inner = pl.multiple_of((group - gathered) * lanes + at, step_u // 2)
                start = pl.multiple_of(group * lanes + at, step_u // 2)
                near, span = pl.ds(inner, step_u // 2), pl.ds(start, step_u // 2)
                scale = jnp.concatenate([sq_u[span, :]] * (wide // lanes), axis=1)
                step = sum_u[span, :] * scale
                tu[span, :] = hold_rate * eu[span, :] + step
                stepped = base_u[near, :] - learn_rate * step
                su[span, :] = stepped
                place = pl.ds(pl.multiple_of(me * rows + start, step_u // 2), step_u // 2)
                cu[place, :] = stepped.astype(cu.dtype)
                scale = jnp.concatenate([sq_o[near, :]] * (wide // lanes), axis=1)
                step = (give_u[near, :] + other_u[0, near, :]) * scale
                stepped = other_u[1, near, :] - learn_rate * step
                place = pl.ds(pl.multiple_of(peer * rows + start, step_u // 2), step_u // 2)
                cu[place, :] = stepped.astype(cu.dtype)

    send_vec.wait_recv()
    mean = (vec[0:2, :] + got_vec[0:2, :]) * rate
    for at, (state, stepped, rounded) in enumerate(((tn, sn, cn), (tb, sb, cb))):
        row = slice(2 + at, 3 + at)
        low, high = mean[at : at + 1, :half], mean[at : at + 1, half:]
        new_own = hold_rate * vec[row, half:] + jnp.where(me == 0, low, high)
        own = vec[row, :half] - learn_rate * new_own
        new_other = hold_rate * got_vec[row, half:] + jnp.where(me == 0, high, low)
        other = got_vec[row, :half] - learn_rate * new_other
        state[...] = new_own.reshape(state.shape)
        stepped[...] = own.reshape(stepped.shape)
        whole = jnp.concatenate(
            [jnp.where(me == 0, own, other), jnp.where(me == 0, other, own)], axis=1
        )
        rounded[...] = whole.reshape(rounded.shape).astype(rounded.dtype)

    @pl.when(me == 0)
    def _():
        wait_for(sum_d.at[last, :], part_sem.at[groups + 2])
        sum_columns(last, None, own_d, sum_d, sum_d)
        wait_for(pack.at[0], more_sem.at[1])

    @pl.when(me == 1)
    def _():
        wait_for(pack.at[0, head, :], more_sem.at[1])

    wait_for(base_d, more_sem.at[4])

    send_vec.wait_send()
    wait_for(stat_u.at[pl.ds(0, gathered * (n - 1))], small_sem.at[1])
    wait_for(stat_w.at[pl.ds(0, (groups - gathered) * (2 * n - 1))], small_sem.at[2])
    wait_for(stat_d.at[pl.ds(0, 2 * n - 1)], small_sem.at[3])
    wait_for(cu.at[at_core(peer, rows, 0, first), :], more_sem.at[3])
    wait_for(pack, send_sem.at[0])


def finish(
    cu_v, cn_v, cb_v, su_v, sn_v, sb_v, tu_v, tn_v, tb_v,
    pack, ed, stat_d,
    cu, cd, cn, cb, su, sd, sn, sb, tu, td, tn, tb,
    cd_v, sd_v, td_v, sem,
):
    me = lax.axis_index("dp")
    rate = lax.axis_size("dp") ** (-0.5)
    n = lax.axis_size("tp")
    tall, cols = td_v.shape
    step = 32
    mine_d, base_o, sum_d, base_d, give_d = (pack.at[at] for at in range(5))

    def out(source, target, at):
        copy = pltpu.make_async_copy(source, target, sem.at[at])
        copy.start()
        return copy

    def vectors(small_sem):
        small = [
            pltpu.make_async_copy(source, target, small_sem.at[at])
            for at, (source, target) in enumerate(
                ((cn_v, cn), (cb_v, cb), (sn_v, sn), (sb_v, sb), (tn_v, tn), (tb_v, tb))
            )
        ]
        for copy in small:
            copy.start()
        matrices()
        for copy in small:
            copy.wait()

    def matrices():
        out(su_v, su, 0)
        out(tu_v, tu, 0)
        out(cu_v, cu, 1)

        scales = []
        for core in (me, 1 - me):
            weights = sizes = 0.0
            for at in range(n):
                near, far = stat_d[core * n + at], stat_d[(1 - core) * n + at]
                weights = weights + near[0:1, :]
                sizes = sizes + near[1:2, :] + far[2:3, :]
            scales.append(scale_of(weights, sizes, rate))
        own, other = scales
        for piece in range(pieces):
            size = tall // pieces

            @blocks(size, step)
            def _(at):
                span = pl.ds(pl.multiple_of(piece * size + at, step), step)
                x = sum_d[span, :] * own
                td_v[span, :] = hold_rate * ed[span, :] + x
                stepped = base_d[span, :] - learn_rate * x
                sd_v[span, :] = stepped
                cd_v[span, pl.ds(pl.multiple_of(me * cols, cols), cols)] = stepped.astype(cd_v.dtype)
                x = (give_d[span, :] + mine_d[span, :]) * other
                stepped = base_o[span, :] - learn_rate * x
                cd_v[span, pl.ds(pl.multiple_of((1 - me) * cols, cols), cols)] = stepped.astype(cd_v.dtype)

            span = pl.ds(piece * size, size)
            out(td_v.at[span, :], td.at[span, :], 0)
            out(sd_v.at[span, :], sd.at[span, :], 0)
            out(cd_v.at[span, :], cd.at[span, :], 0)

    pl.run_scoped(vectors, pltpu.SemaphoreType.DMA((6,)))
    wait_for(cu_v, sem.at[1])
    wait_for(pack, sem.at[0])


def held(arrays):
    return [pltpu.with_memory_space_constraint(x, pltpu.HBM) for x in arrays]


def on_pair(*args):
    pu, pd, pn, pb, mu, md, mn, mb, eu, ed, en, eb = args
    n = lax.axis_size("tp")
    f32, bf16 = jnp.float32, jnp.bfloat16
    vmem = pl.BlockSpec(memory_space=pltpu.VMEM)
    hbm = pl.BlockSpec(memory_space=pltpu.HBM)
    wide, tall = pu.shape[2], pd.shape[1]
    rows, cols = mu.shape[0], md.shape[1]
    groups = rows // lanes
    rest = rows - gathered * lanes
    dma = pltpu.SemaphoreType.DMA

    def shaped(shape, dtype=f32):
        return jax.ShapeDtypeStruct(shape, dtype)

    between = [
        shaped((pu.shape[1], wide), bf16), shaped((pn.shape[1],), bf16), shaped((pb.shape[1],), bf16),
        *(shaped(x.shape) for x in (mu, mn, mb)),
        *(shaped(x.shape) for x in (mu, mn, mb)),
        shaped((5, *md.shape)),
        shaped(md.shape),
        shaped((2 * n, 4, cols)),
    ]
    results = pl.pallas_call(
        exchange,
        out_shape=between,
        in_specs=[hbm] * len(args),
        out_specs=[vmem] * len(between),
        scratch_shapes=[
            pltpu.VMEM(mu.shape, f32),
            pltpu.VMEM(md.shape, f32),
            pltpu.VMEM((rest, wide), f32),
            pltpu.VMEM(mu.shape, f32),
            pltpu.VMEM((rest, wide), f32),
            pltpu.VMEM((2, rest, wide), f32),
            *(pltpu.VMEM(x.shape, f32) for x in (mu, md, mu)),
            *(pltpu.VMEM(x.shape, f32) for x in (pn, pb, mn, mb, en, eb)),
            pltpu.VMEM((4, pn.shape[1]), f32),
            pltpu.VMEM((4, pn.shape[1]), f32),
            pltpu.VMEM((rows, lanes), f32),
            pltpu.VMEM((rest, lanes), f32),
            pltpu.VMEM((8, cols), f32),
            pltpu.VMEM((8, cols), f32),
            pltpu.VMEM((gathered * n, 2, lanes), f32),
            pltpu.VMEM(((groups - gathered) * 2 * n, 2, lanes), f32),
            dma((1,)),
        ],
        compiler_params=pltpu.CompilerParams(
            collective_id=0, has_side_effects=True, vmem_limit_bytes=40 * 2**20
        ),
        name="exchange",
    )(*held((pu[0], pd[0], *args[2:])))
    outs = (
        ((pu.shape[1], wide), bf16),
        ((tall, pd.shape[2]), bf16),
        ((pn.shape[1],), bf16),
        ((pb.shape[1],), bf16),
        *((x.shape, f32) for x in (mu, md, mn, mb)),
        *((x.shape, f32) for x in (mu, md, mn, mb)),
    )
    return tuple(pl.pallas_call(
        finish,
        out_shape=[shaped(shape, dtype) for shape, dtype in outs],
        in_specs=[vmem] * len(between),
        out_specs=[hbm] * len(outs),
        scratch_shapes=[
            pltpu.VMEM((tall, pd.shape[2]), bf16),
            pltpu.VMEM(md.shape, f32),
            pltpu.VMEM(md.shape, f32),
            dma((2,)),
        ],
        compiler_params=pltpu.CompilerParams(vmem_limit_bytes=8 * 2**20),
        name="finish",
    )(*results))


def solution(mesh):
    in_specs = (
        P(("job", "dp"), None, "tp"),
        P(("job", "dp"), "tp", None),
        P(("job", "dp"), None),
        P(("job", "dp"), None),
        P(("job", "dp"), "tp"),
        P(("job", "tp"), "dp"),
        P(("job", "dp")),
        P(("job", "dp")),
        P(("job", "dp"), "tp"),
        P(("job", "tp"), "dp"),
        P(("job", "dp")),
        P(("job", "dp")),
    )
    out_specs = (
        P("job", "tp"),
        P(("job", "tp"), None),
        P("job"),
        P("job"),
        P(("job", "dp"), "tp"),
        P(("job", "tp"), "dp"),
        P(("job", "dp")),
        P(("job", "dp")),
        P(("job", "dp"), "tp"),
        P(("job", "tp"), "dp"),
        P(("job", "dp")),
        P(("job", "dp")),
    )
    return jax.shard_map(
        on_device if mesh.shape["dp"] != 2 else on_pair, mesh=mesh, in_specs=in_specs, out_specs=out_specs, check_vma=False
    )
```

```python
import functools

import jax
import jax.numpy as jnp
from jax import lax
from jax.experimental import pallas as pl
from jax.experimental.pallas import tpu as pltpu
from jax.sharding import PartitionSpec as P

learn_rate = 0.4
hold_rate = 0.9


def on_device(
    partial_up,
    partial_down,
    partial_norm,
    partial_bias,
    master_up,
    master_down,
    master_norm,
    master_bias,
    memory_up,
    memory_down,
    memory_norm,
    memory_bias,
):
    mean_up, mean_down = (
        lax.psum_scatter(partial_up[0], "dp", scatter_dimension=0, tiled=True),
        lax.psum_scatter(partial_down[0], "dp", scatter_dimension=1, tiled=True),
    )
    whole_norm, whole_bias = lax.psum((partial_norm[0], partial_bias[0]), "dp")
    place = lax.axis_index("dp")
    mean_norm = lax.dynamic_slice_in_dim(
        whole_norm, place * master_norm.shape[0], master_norm.shape[0]
    )
    mean_bias = lax.dynamic_slice_in_dim(
        whole_bias, place * master_bias.shape[0], master_bias.shape[0]
    )
    mean_rate = lax.axis_size("dp") ** (-0.5)
    mean_up = mean_up * mean_rate
    mean_down = mean_down * mean_rate
    mean_norm = mean_norm * mean_rate
    mean_bias = mean_bias * mean_rate
    own_up, own_down, slope_up_norm, slope_down_norm = lax.psum(
        (
            jnp.sum(master_up * master_up, axis=1, keepdims=True),
            jnp.sum(master_down * master_down, axis=0, keepdims=True),
            jnp.sum(mean_up * mean_up, axis=1, keepdims=True),
            jnp.sum(mean_down * mean_down, axis=0, keepdims=True),
        ),
        "tp",
    )
    mean_up = mean_up * (jnp.sqrt(own_up) * lax.rsqrt(slope_up_norm + 1e-06))
    mean_down = mean_down * (jnp.sqrt(own_down) * lax.rsqrt(slope_down_norm + 1e-06))
    state_new_up = hold_rate * memory_up + mean_up
    stepped_up = master_up - learn_rate * state_new_up
    state_new_down = hold_rate * memory_down + mean_down
    stepped_down = master_down - learn_rate * state_new_down
    state_new_norm = hold_rate * memory_norm + mean_norm
    stepped_norm = master_norm - learn_rate * state_new_norm
    state_new_bias = hold_rate * memory_bias + mean_bias
    stepped_bias = master_bias - learn_rate * state_new_bias
    compute_up, compute_down, compute_norm, compute_bias = (
        lax.all_gather(stepped_up.astype(jnp.bfloat16), "dp", axis=0, tiled=True),
        lax.all_gather(stepped_down.astype(jnp.bfloat16), "dp", axis=1, tiled=True),
        lax.all_gather(stepped_norm.astype(jnp.bfloat16), "dp", axis=0, tiled=True),
        lax.all_gather(stepped_bias.astype(jnp.bfloat16), "dp", axis=0, tiled=True),
    )
    return (
        compute_up,
        compute_down,
        compute_norm,
        compute_bias,
        stepped_up,
        stepped_down,
        stepped_norm,
        stepped_bias,
        state_new_up,
        state_new_down,
        state_new_norm,
        state_new_bias,
    )


pieces = 4
lanes = 128
gathered = 2


def lane_sums(x):
    total = x[:, :lanes]
    for at in range(lanes, x.shape[1], lanes):
        total = total + x[:, at : at + lanes]
    return total


def blocks(count, step):
    def over(body):
        @pl.loop(0, count // step)
        def _(at):
            body(pl.multiple_of(at * step, step))

    return over


def wait_for(ref, sem):
    pltpu.make_async_copy(ref, ref, sem).wait()


def scale_of(weights, sizes, rate):
    return jnp.sqrt(weights) * (lax.rsqrt(sizes * (rate * rate) + 1e-06) * rate)


def scale_at(stat, first, n, rate):
    total = stat[first]
    for at in range(1, n):
        total = total + stat[first + at]
    return scale_of(total[0:1, :], total[1:2, :], rate)


def exchange(*refs):
    groups = refs[4].shape[0] // lanes
    dma, regular = pltpu.SemaphoreType.DMA, pltpu.SemaphoreType.REGULAR
    pl.run_scoped(
        functools.partial(exchange_in_scope, *refs),
        dma((2,)), dma((6,)), dma((groups + 7,)), dma((1,)), dma((groups + 1,)), dma((5,)), regular, regular,
    )


def exchange_in_scope(
    pu, pd, pn, pb, mu_h, md_h, mn, mb, eu_h, ed_h, en, eb,
    cu, cn, cb, su, sn, sb, tu, tn, tb,
    pack, ed, stat_d,
    own_u, own_d, give_u, sum_u, base_u, other_u, mu, md, eu,
    pn_v, pb_v, mn_v, mb_v, en_v, eb_v, vec, got_vec,
    sq_u, sq_o, acc_d, acc_o, stat_u, stat_w,
    load_sem, small_sem, part_sem, send_sem, stat_sem, more_sem, hello, ready,
):
    me = lax.axis_index("dp")
    peer = 1 - me
    here = lax.axis_index("tp")
    n = lax.axis_size("tp")
    rate = lax.axis_size("dp") ** (-0.5)
    rows, wide = mu.shape
    tall, cols = md.shape
    groups = rows // lanes
    step_u, step_d = 32, 64
    shared = 5 * tall // 24 // 32 * 32
    other_d, (sum_d, base_d, give_d) = pack.at[pl.ds(0, 2)], (pack.at[at] for at in range(2, 5))
    first = gathered * lanes
    rest = pl.ds(first, rows - first)

    def at_core(core, size, start=0, count=None):
        return pl.ds(pl.multiple_of(core * size + start, 8), size if count is None else count)

    def columns(core):
        return pl.ds(pl.multiple_of(core * cols, cols), cols)

    def load(source, target, sem):
        copy = pltpu.make_async_copy(source, target, sem)
        copy.start()
        return copy

    small = [
        load(source, target, small_sem.at[at])
        for at, (source, target) in enumerate(
            ((pn, pn_v), (pb, pb_v), (mn, mn_v), (mb, mb_v), (en, en_v), (eb, eb_v))
        )
    ]
    load(pu.at[at_core(me, rows), :], own_u, load_sem.at[0])
    load(mu_h, mu, load_sem.at[0])

    barrier = pltpu.get_barrier_semaphore()

    @pl.when(me == 1)
    def _():
        pl.semaphore_signal(barrier, inc=1, device_id={"dp": peer})

    @pl.when(me == 0)
    def _():
        pl.semaphore_wait(barrier, 1)
        pl.semaphore_signal(hello, inc=1, device_id={"dp": peer})

    @pl.when(me == 1)
    def _():
        pl.semaphore_wait(hello, 1)
        for step in range(1, n):
            pl.semaphore_signal(barrier, inc=1, device_id={"tp": lax.rem(here + step, n)})

    def to_peer(source, target, send, recv):
        copy = pltpu.make_async_remote_copy(
            src_ref=source, dst_ref=target, send_sem=send, recv_sem=recv, device_id={"dp": peer}
        )
        copy.start()
        return copy

    def ending(start, size):
        return [pl.ds(start, size - step_u), pl.ds(start + size - step_u, step_u)]

    spans_u = [pl.ds(at * lanes, lanes) for at in range(groups)]
    head, last = pl.ds(0, tall - shared), pl.ds(tall - shared, shared)
    heads = [pl.ds(0, tall - 2 * shared), *ending(tall - 2 * shared, shared)]
    lasts = ending(tall - shared, shared)
    sent = [
        to_peer(pu.at[at_core(peer, rows, at * lanes, lanes), :], sum_u.at[span, :], send_sem.at[0], part_sem.at[at])
        for at, span in enumerate(spans_u)
    ]
    for at, span in enumerate(heads):
        sent.append(to_peer(pd.at[span, columns(peer)], sum_d.at[span, :], send_sem.at[0], part_sem.at[groups + at]))

    @pl.when(me == 0)
    def _():
        for at, span in enumerate(lasts):
            to_peer(pd.at[span, columns(peer)], sum_d.at[span, :], send_sem.at[0], part_sem.at[groups + 3 + at])
        for at, span in enumerate(lasts):
            to_peer(pd.at[span, columns(me)], other_d.at[0, span, :], send_sem.at[0], part_sem.at[groups + 5 + at])

    load(md_h, md, load_sem.at[1])
    load(ed_h, ed, load_sem.at[1])
    load(eu_h, eu, load_sem.at[1])
    load(pd.at[:, columns(me)], own_d, load_sem.at[1])

    wait_for(other_d, load_sem.at[0])
    load(pd.at[:, columns(peer)], give_d, load_sem.at[0])
    for copy in small:
        copy.wait()
    load(pu.at[at_core(peer, rows, first, rows - first), :], give_u, small_sem.at[0])

    @blocks(rows, step_u)
    def _(at):
        span = pl.ds(at, step_u)
        x = mu[span, :]
        sq_u[span, :] = lane_sums(x * x)

    def store_size(group, which):
        size = jnp.sum(sq_u[spans_u[group], :].T, axis=0).reshape(1, 1, lanes)
        if group < gathered:
            stat_u[pl.ds(group * n + here, 1), which : which + 1, :] = size
        else:
            at = (2 * (group - gathered) + me) * n + here
            stat_w[pl.ds(at, 1), which : which + 1, :] = size

    for group in range(groups):
        store_size(group, 0)

    def sizes(ref, at, send, recv, cores):
        for step in (*range(1, n), 0):
            for core in range(cores):
                if step + core > 0:
                    target = me if cores == 1 else core if step else peer
                    pltpu.make_async_remote_copy(
                        src_ref=ref.at[at],
                        dst_ref=ref.at[at],
                        send_sem=small_sem.at[send],
                        recv_sem=recv,
                        device_id={"dp": target, "tp": lax.rem(here + step, n)},
                    ).start()

    def sum_rows(group):
        sent[group].wait_recv()

        @blocks(lanes, step_u)
        def _(at):
            span = pl.ds(pl.multiple_of(group * lanes + at, step_u), step_u)
            x = own_u[span, :] + sum_u[span, :]
            sum_u[span, :] = x
            sq_u[span, :] = lane_sums(x * x)

        store_size(group, 1)

    def send_sizes(group):
        if group < gathered:
            sizes(stat_u, group * n + here, 1, stat_sem.at[group], 1)
        else:
            sizes(stat_w, (2 * (group - gathered) + me) * n + here, 2, stat_sem.at[group], 2)

    def meet():
        @pl.when(me == 1)
        def _():
            pl.semaphore_wait(barrier, n - 1)
            pl.semaphore_signal(ready, inc=1, device_id={"dp": peer})

        @pl.when(me == 0)
        def _():
            pl.semaphore_wait(ready, 1)

    for group in range(groups - 1):
        sum_rows(group)

        @pl.when(2 * here >= n)
        def _(group=group):
            if group == 0:
                meet()
            send_sizes(group)

    half = mn.shape[-1]
    vec[0:1, :] = pn_v[...]
    vec[1:2, :] = pb_v[...]
    vec[2:3, :half] = mn_v[...].reshape(1, half)
    vec[2:3, half:] = en_v[...].reshape(1, half)
    vec[3:4, :half] = mb_v[...].reshape(1, half)
    vec[3:4, half:] = eb_v[...].reshape(1, half)
    send_vec = to_peer(vec, got_vec, small_sem.at[4], more_sem.at[2])

    wait_for(pack.at[pl.ds(0, 4)], load_sem.at[1])
    acc_d[...] = jnp.zeros_like(acc_d)
    acc_o[...] = jnp.zeros_like(acc_o)

    def eighths(x):
        return jnp.sum(x.reshape(x.shape[0] // 8, 8, cols), axis=0)

    @blocks(tall, step_d)
    def _(at):
        span = pl.ds(at, step_d)
        x = md[span, :]
        base_d[span, :] = x - (learn_rate * hold_rate) * ed[span, :]
        acc_d[...] += eighths(x * x)

    slot_d = me * n + here
    stat_d[pl.ds(slot_d, 1), :, :] = jnp.broadcast_to(jnp.sum(acc_d[...], axis=0).reshape(1, 1, cols), (1, 4, cols))
    acc_d[...] = jnp.zeros_like(acc_d)

    @blocks(rows - first, step_u)
    def _(at):
        span = pl.ds(pl.multiple_of(first + at, step_u), step_u)
        base_u[pl.ds(at, step_u), :] = mu[span, :] - (learn_rate * hold_rate) * eu[span, :]

    to_peer(own_u.at[rest, :], other_u.at[0], send_sem.at[0], more_sem.at[0])
    to_peer(base_u, other_u.at[1], send_sem.at[0], more_sem.at[0])

    @pl.when(me == 0)
    def _():
        to_peer(own_d.at[head, :], other_d.at[0, head, :], send_sem.at[0], more_sem.at[1])

    @pl.when(me == 1)
    def _():
        to_peer(own_d, other_d.at[0], send_sem.at[0], more_sem.at[1])
        to_peer(pd.at[last, columns(peer)], sum_d.at[last, :], send_sem.at[0], part_sem.at[groups + 3])

    to_peer(base_d, other_d.at[1], send_sem.at[0], more_sem.at[4])

    @pl.when(2 * here < n)
    def _():
        meet()
        for group in range(groups - 1):
            send_sizes(group)

    sum_rows(groups - 1)
    send_sizes(groups - 1)

    def sum_columns(part, acc, one, two, total=None):
        step = step_d if part.size % step_d == 0 else 32

        @blocks(part.size, step)
        def _(at):
            span = pl.ds(pl.multiple_of(part.start + at, 32), step)
            x = one[span, :] + two[span, :]
            if total is not None:
                total[span, :] = x
            if acc is not None:
                acc[...] += eighths(x * x)

    wait_for(give_d, load_sem.at[0])
    for at, span in enumerate(heads):
        sent[groups + at].wait_recv()
        sum_columns(span, acc_d, own_d, sum_d, sum_d)

    @pl.when(me == 1)
    def _():
        for at, span in enumerate(lasts):
            wait_for(sum_d.at[span, :], part_sem.at[groups + 3 + at])
            sum_columns(span, acc_d, own_d, sum_d, sum_d)
        for at, span in enumerate(lasts):
            wait_for(sum_d.at[span, :], part_sem.at[groups + 5 + at])
            sum_columns(span, acc_o, give_d, other_d.at[0])

    stat_d[pl.ds(slot_d, 1), 1:2, :] = jnp.sum(acc_d[...], axis=0).reshape(1, 1, cols)
    stat_d[pl.ds(slot_d, 1), 2:3, :] = jnp.sum(acc_o[...], axis=0).reshape(1, 1, cols)
    sizes(stat_d, slot_d, 3, stat_sem.at[groups], 2)

    for group in range(groups):
        span = spans_u[group]
        if group < gathered:
            wait_for(stat_u.at[pl.ds(0, n - 1)], stat_sem.at[group])
            sq_u[span, :] = jnp.broadcast_to(scale_at(stat_u, group * n, n, rate), (lanes, lanes)).T
        else:
            wait_for(stat_w.at[pl.ds(0, 2 * n - 1)], stat_sem.at[group])
            at = 2 * (group - gathered)
            sq_u[span, :] = jnp.broadcast_to(scale_at(stat_w, (at + me) * n, n, rate), (lanes, lanes)).T
            sq_o[pl.ds((group - gathered) * lanes, lanes), :] = jnp.broadcast_to(
                scale_at(stat_w, (at + peer) * n, n, rate), (lanes, lanes)
            ).T
        if group < gathered:

            @blocks(lanes, step_u)
            def _(at):
                start = pl.multiple_of(group * lanes + at, step_u)
                span = pl.ds(start, step_u)
                scale = jnp.concatenate([sq_u[span, :]] * (wide // lanes), axis=1)
                state = hold_rate * eu[span, :] + sum_u[span, :] * scale
                stepped = mu[span, :] - learn_rate * state
                tu[span, :] = state
                su[span, :] = stepped
                cu[pl.ds(pl.multiple_of(me * rows + start, step_u), step_u), :] = stepped.astype(cu.dtype)

            part = cu.at[at_core(me, rows, group * lanes, lanes), :]
            to_peer(part, part, send_sem.at[0], more_sem.at[3])
        else:
            if group == gathered:
                wait_for(other_u, more_sem.at[0])
                wait_for(give_u, small_sem.at[0])

            @blocks(lanes, step_u // 2)
            def _(at):
                inner = pl.multiple_of((group - gathered) * lanes + at, step_u // 2)
                start = pl.multiple_of(group * lanes + at, step_u // 2)
                near, span = pl.ds(inner, step_u // 2), pl.ds(start, step_u // 2)
                scale = jnp.concatenate([sq_u[span, :]] * (wide // lanes), axis=1)
                step = sum_u[span, :] * scale
                tu[span, :] = hold_rate * eu[span, :] + step
                stepped = base_u[near, :] - learn_rate * step
                su[span, :] = stepped
                place = pl.ds(pl.multiple_of(me * rows + start, step_u // 2), step_u // 2)
                cu[place, :] = stepped.astype(cu.dtype)
                scale = jnp.concatenate([sq_o[near, :]] * (wide // lanes), axis=1)
                step = (give_u[near, :] + other_u[0, near, :]) * scale
                stepped = other_u[1, near, :] - learn_rate * step
                place = pl.ds(pl.multiple_of(peer * rows + start, step_u // 2), step_u // 2)
                cu[place, :] = stepped.astype(cu.dtype)

    send_vec.wait_recv()
    mean = (vec[0:2, :] + got_vec[0:2, :]) * rate
    for at, (state, stepped, rounded) in enumerate(((tn, sn, cn), (tb, sb, cb))):
        row = slice(2 + at, 3 + at)
        low, high = mean[at : at + 1, :half], mean[at : at + 1, half:]
        new_own = hold_rate * vec[row, half:] + jnp.where(me == 0, low, high)
        own = vec[row, :half] - learn_rate * new_own
        new_other = hold_rate * got_vec[row, half:] + jnp.where(me == 0, high, low)
        other = got_vec[row, :half] - learn_rate * new_other
        state[...] = new_own.reshape(state.shape)
        stepped[...] = own.reshape(stepped.shape)
        whole = jnp.concatenate(
            [jnp.where(me == 0, own, other), jnp.where(me == 0, other, own)], axis=1
        )
        rounded[...] = whole.reshape(rounded.shape).astype(rounded.dtype)

    @pl.when(me == 0)
    def _():
        wait_for(sum_d.at[last, :], part_sem.at[groups + 3])
        sum_columns(last, None, own_d, sum_d, sum_d)
        wait_for(pack.at[0], more_sem.at[1])

    @pl.when(me == 1)
    def _():
        wait_for(pack.at[0, head, :], more_sem.at[1])

    wait_for(base_d, more_sem.at[4])

    send_vec.wait_send()
    wait_for(stat_u.at[pl.ds(0, gathered * (n - 1))], small_sem.at[1])
    wait_for(stat_w.at[pl.ds(0, (groups - gathered) * (2 * n - 1))], small_sem.at[2])
    wait_for(stat_d.at[pl.ds(0, 2 * n - 1)], small_sem.at[3])
    wait_for(stat_d.at[pl.ds(0, 2 * n - 1)], stat_sem.at[groups])
    wait_for(cu.at[at_core(peer, rows, 0, first), :], more_sem.at[3])
    wait_for(pack, send_sem.at[0])


def finish(
    cu_v, cn_v, cb_v, su_v, sn_v, sb_v, tu_v, tn_v, tb_v,
    pack, ed, stat_d,
    cu, cd, cn, cb, su, sd, sn, sb, tu, td, tn, tb,
    cd_v, sd_v, td_v,
):
    me = lax.axis_index("dp")
    rate = lax.axis_size("dp") ** (-0.5)
    n = lax.axis_size("tp")
    tall, cols = td_v.shape
    step = 32
    mine_d, base_o, sum_d, base_d, give_d = (pack.at[at] for at in range(5))

    def out(source, target, sem):
        copy = pltpu.make_async_copy(source, target, sem)
        copy.start()
        return copy

    def write(sem):
        small = [
            pltpu.make_async_copy(source, target, sem.at[2 + at])
            for at, (source, target) in enumerate(
                ((cn_v, cn), (cb_v, cb), (sn_v, sn), (sb_v, sb), (tn_v, tn), (tb_v, tb))
            )
        ]
        for copy in small:
            copy.start()
        matrices(sem)
        for copy in small:
            copy.wait()
        wait_for(cu_v, sem.at[1])
        wait_for(pack, sem.at[0])

    def matrices(sem):
        out(su_v, su, sem.at[0])
        out(tu_v, tu, sem.at[0])
        out(cu_v, cu, sem.at[1])

        scales = []
        for core in (me, 1 - me):
            weights = sizes = 0.0
            for at in range(n):
                near, far = stat_d[core * n + at], stat_d[(1 - core) * n + at]
                weights = weights + near[0:1, :]
                sizes = sizes + near[1:2, :] + far[2:3, :]
            scales.append(scale_of(weights, sizes, rate))
        own, other = scales
        for piece in range(pieces):
            size = tall // pieces

            @blocks(size, step)
            def _(at):
                span = pl.ds(pl.multiple_of(piece * size + at, step), step)
                x = sum_d[span, :] * own
                td_v[span, :] = hold_rate * ed[span, :] + x
                stepped = base_d[span, :] - learn_rate * x
                sd_v[span, :] = stepped
                cd_v[span, pl.ds(pl.multiple_of(me * cols, cols), cols)] = stepped.astype(cd_v.dtype)
                x = (give_d[span, :] + mine_d[span, :]) * other
                stepped = base_o[span, :] - learn_rate * x
                cd_v[span, pl.ds(pl.multiple_of((1 - me) * cols, cols), cols)] = stepped.astype(cd_v.dtype)

            span = pl.ds(piece * size, size)
            out(td_v.at[span, :], td.at[span, :], sem.at[0])
            out(sd_v.at[span, :], sd.at[span, :], sem.at[0])
            out(cd_v.at[span, :], cd.at[span, :], sem.at[0])

    pl.run_scoped(write, pltpu.SemaphoreType.DMA((8,)))


def held(arrays):
    return [pltpu.with_memory_space_constraint(x, pltpu.HBM) for x in arrays]


def on_pair(*args):
    pu, pd, pn, pb, mu, md, mn, mb, eu, ed, en, eb = args
    n = lax.axis_size("tp")
    f32, bf16 = jnp.float32, jnp.bfloat16
    vmem = pl.BlockSpec(memory_space=pltpu.VMEM)
    hbm = pl.BlockSpec(memory_space=pltpu.HBM)
    wide, tall = pu.shape[2], pd.shape[1]
    rows, cols = mu.shape[0], md.shape[1]
    groups = rows // lanes
    rest = rows - gathered * lanes

    def shaped(shape, dtype=f32):
        return jax.ShapeDtypeStruct(shape, dtype)

    between = [
        shaped((pu.shape[1], wide), bf16), shaped((pn.shape[1],), bf16), shaped((pb.shape[1],), bf16),
        *(shaped(x.shape) for x in (mu, mn, mb)),
        *(shaped(x.shape) for x in (mu, mn, mb)),
        shaped((5, *md.shape)),
        shaped(md.shape),
        shaped((2 * n, 4, cols)),
    ]
    results = pl.pallas_call(
        exchange,
        out_shape=between,
        in_specs=[hbm] * len(args),
        out_specs=[vmem] * len(between),
        scratch_shapes=[
            pltpu.VMEM(mu.shape, f32),
            pltpu.VMEM(md.shape, f32),
            pltpu.VMEM((rest, wide), f32),
            pltpu.VMEM(mu.shape, f32),
            pltpu.VMEM((rest, wide), f32),
            pltpu.VMEM((2, rest, wide), f32),
            *(pltpu.VMEM(x.shape, f32) for x in (mu, md, mu)),
            *(pltpu.VMEM(x.shape, f32) for x in (pn, pb, mn, mb, en, eb)),
            pltpu.VMEM((4, pn.shape[1]), f32),
            pltpu.VMEM((4, pn.shape[1]), f32),
            pltpu.VMEM((rows, lanes), f32),
            pltpu.VMEM((rest, lanes), f32),
            pltpu.VMEM((8, cols), f32),
            pltpu.VMEM((8, cols), f32),
            pltpu.VMEM((gathered * n, 2, lanes), f32),
            pltpu.VMEM(((groups - gathered) * 2 * n, 2, lanes), f32),
        ],
        compiler_params=pltpu.CompilerParams(
            collective_id=0, has_side_effects=True, vmem_limit_bytes=40 * 2**20
        ),
        name="exchange",
    )(*held((pu[0], pd[0], *args[2:])))
    outs = (
        ((pu.shape[1], wide), bf16),
        ((tall, pd.shape[2]), bf16),
        ((pn.shape[1],), bf16),
        ((pb.shape[1],), bf16),
        *((x.shape, f32) for x in (mu, md, mn, mb)),
        *((x.shape, f32) for x in (mu, md, mn, mb)),
    )
    return tuple(pl.pallas_call(
        finish,
        out_shape=[shaped(shape, dtype) for shape, dtype in outs],
        in_specs=[vmem] * len(between),
        out_specs=[hbm] * len(outs),
        scratch_shapes=[
            pltpu.VMEM((tall, pd.shape[2]), bf16),
            pltpu.VMEM(md.shape, f32),
            pltpu.VMEM(md.shape, f32),
        ],
        compiler_params=pltpu.CompilerParams(vmem_limit_bytes=8 * 2**20),
        name="finish",
    )(*results))


def solution(mesh):
    in_specs = (
        P(("job", "dp"), None, "tp"),
        P(("job", "dp"), "tp", None),
        P(("job", "dp"), None),
        P(("job", "dp"), None),
        P(("job", "dp"), "tp"),
        P(("job", "tp"), "dp"),
        P(("job", "dp")),
        P(("job", "dp")),
        P(("job", "dp"), "tp"),
        P(("job", "tp"), "dp"),
        P(("job", "dp")),
        P(("job", "dp")),
    )
    out_specs = (
        P("job", "tp"),
        P(("job", "tp"), None),
        P("job"),
        P("job"),
        P(("job", "dp"), "tp"),
        P(("job", "tp"), "dp"),
        P(("job", "dp")),
        P(("job", "dp")),
        P(("job", "dp"), "tp"),
        P(("job", "tp"), "dp"),
        P(("job", "dp")),
        P(("job", "dp")),
    )
    return jax.shard_map(
        on_device if mesh.shape["dp"] != 2 else on_pair, mesh=mesh, in_specs=in_specs, out_specs=out_specs, check_vma=False
    )
```

```python
import functools

import jax
import jax.numpy as jnp
from jax import lax
from jax.experimental import pallas as pl
from jax.experimental.pallas import tpu as pltpu
from jax.sharding import PartitionSpec as P

learn_rate = 0.4
hold_rate = 0.9


def on_device(
    partial_up,
    partial_down,
    partial_norm,
    partial_bias,
    master_up,
    master_down,
    master_norm,
    master_bias,
    memory_up,
    memory_down,
    memory_norm,
    memory_bias,
):
    mean_up, mean_down = (
        lax.psum_scatter(partial_up[0], "dp", scatter_dimension=0, tiled=True),
        lax.psum_scatter(partial_down[0], "dp", scatter_dimension=1, tiled=True),
    )
    whole_norm, whole_bias = lax.psum((partial_norm[0], partial_bias[0]), "dp")
    place = lax.axis_index("dp")
    mean_norm = lax.dynamic_slice_in_dim(
        whole_norm, place * master_norm.shape[0], master_norm.shape[0]
    )
    mean_bias = lax.dynamic_slice_in_dim(
        whole_bias, place * master_bias.shape[0], master_bias.shape[0]
    )
    mean_rate = lax.axis_size("dp") ** (-0.5)
    mean_up = mean_up * mean_rate
    mean_down = mean_down * mean_rate
    mean_norm = mean_norm * mean_rate
    mean_bias = mean_bias * mean_rate
    own_up, own_down, slope_up_norm, slope_down_norm = lax.psum(
        (
            jnp.sum(master_up * master_up, axis=1, keepdims=True),
            jnp.sum(master_down * master_down, axis=0, keepdims=True),
            jnp.sum(mean_up * mean_up, axis=1, keepdims=True),
            jnp.sum(mean_down * mean_down, axis=0, keepdims=True),
        ),
        "tp",
    )
    mean_up = mean_up * (jnp.sqrt(own_up) * lax.rsqrt(slope_up_norm + 1e-06))
    mean_down = mean_down * (jnp.sqrt(own_down) * lax.rsqrt(slope_down_norm + 1e-06))
    state_new_up = hold_rate * memory_up + mean_up
    stepped_up = master_up - learn_rate * state_new_up
    state_new_down = hold_rate * memory_down + mean_down
    stepped_down = master_down - learn_rate * state_new_down
    state_new_norm = hold_rate * memory_norm + mean_norm
    stepped_norm = master_norm - learn_rate * state_new_norm
    state_new_bias = hold_rate * memory_bias + mean_bias
    stepped_bias = master_bias - learn_rate * state_new_bias
    compute_up, compute_down, compute_norm, compute_bias = (
        lax.all_gather(stepped_up.astype(jnp.bfloat16), "dp", axis=0, tiled=True),
        lax.all_gather(stepped_down.astype(jnp.bfloat16), "dp", axis=1, tiled=True),
        lax.all_gather(stepped_norm.astype(jnp.bfloat16), "dp", axis=0, tiled=True),
        lax.all_gather(stepped_bias.astype(jnp.bfloat16), "dp", axis=0, tiled=True),
    )
    return (
        compute_up,
        compute_down,
        compute_norm,
        compute_bias,
        stepped_up,
        stepped_down,
        stepped_norm,
        stepped_bias,
        state_new_up,
        state_new_down,
        state_new_norm,
        state_new_bias,
    )


pieces = 4
lanes = 128
gathered = 2


def lane_sums(x):
    total = x[:, :lanes]
    for at in range(lanes, x.shape[1], lanes):
        total = total + x[:, at : at + lanes]
    return total


def blocks(count, step):
    def over(body):
        @pl.loop(0, count // step)
        def _(at):
            body(pl.multiple_of(at * step, step))

    return over


def wait_for(ref, sem):
    pltpu.make_async_copy(ref, ref, sem).wait()


def scale_of(weights, sizes, rate):
    return jnp.sqrt(weights) * (lax.rsqrt(sizes * (rate * rate) + 1e-06) * rate)


def scale_at(stat, first, n, rate):
    total = stat[first]
    for at in range(1, n):
        total = total + stat[first + at]
    return scale_of(total[0:1, :], total[1:2, :], rate)


def exchange(*refs):
    groups = refs[4].shape[0] // lanes
    dma, regular = pltpu.SemaphoreType.DMA, pltpu.SemaphoreType.REGULAR
    pl.run_scoped(
        functools.partial(exchange_in_scope, *refs),
        dma((2,)), dma((6,)), dma((groups + 7,)), dma((1,)), dma((groups + 2,)), dma((5,)), regular, regular,
    )


def exchange_in_scope(
    pu, pd, pn, pb, mu_h, md_h, mn, mb, eu_h, ed_h, en, eb,
    cu, cn, cb, su, sn, sb, tu, tn, tb,
    pack, ed, stat_d, stat_m,
    own_u, own_d, give_u, sum_u, base_u, other_u, mu, md, eu,
    pn_v, pb_v, mn_v, mb_v, en_v, eb_v, vec, got_vec,
    sq_u, sq_o, acc_d, acc_o, stat_u, stat_w,
    load_sem, small_sem, part_sem, send_sem, stat_sem, more_sem, hello, ready,
):
    me = lax.axis_index("dp")
    peer = 1 - me
    here = lax.axis_index("tp")
    n = lax.axis_size("tp")
    rate = lax.axis_size("dp") ** (-0.5)
    rows, wide = mu.shape
    tall, cols = md.shape
    groups = rows // lanes
    step_u, step_d = 32, 64
    shared = 5 * tall // 24 // 32 * 32
    other_d, (sum_d, base_d, give_d) = pack.at[pl.ds(0, 2)], (pack.at[at] for at in range(2, 5))
    first = gathered * lanes
    rest = pl.ds(first, rows - first)

    def at_core(core, size, start=0, count=None):
        return pl.ds(pl.multiple_of(core * size + start, 8), size if count is None else count)

    def columns(core):
        return pl.ds(pl.multiple_of(core * cols, cols), cols)

    def load(source, target, sem):
        copy = pltpu.make_async_copy(source, target, sem)
        copy.start()
        return copy

    barrier = pltpu.get_barrier_semaphore()

    @pl.when(me == 1)
    def _():
        pl.semaphore_signal(barrier, inc=1, device_id={"dp": peer})

    @pl.when(me == 0)
    def _():
        pl.semaphore_wait(barrier, 1)
        pl.semaphore_signal(hello, inc=1, device_id={"dp": peer})

    small = [
        load(source, target, small_sem.at[at])
        for at, (source, target) in enumerate(
            ((pn, pn_v), (pb, pb_v), (mn, mn_v), (mb, mb_v), (en, en_v), (eb, eb_v))
        )
    ]
    load(pu.at[at_core(me, rows), :], own_u, load_sem.at[0])
    load(mu_h, mu, load_sem.at[0])

    @pl.when(me == 1)
    def _():
        pl.semaphore_wait(hello, 1)
        for step in range(1, n):
            pl.semaphore_signal(barrier, inc=1, device_id={"tp": lax.rem(here + step, n)})

    def to_peer(source, target, send, recv):
        copy = pltpu.make_async_remote_copy(
            src_ref=source, dst_ref=target, send_sem=send, recv_sem=recv, device_id={"dp": peer}
        )
        copy.start()
        return copy

    def ending(start, size):
        return [pl.ds(start, size - step_u), pl.ds(start + size - step_u, step_u)]

    spans_u = [pl.ds(at * lanes, lanes) for at in range(groups)]
    head, last = pl.ds(0, tall - shared), pl.ds(tall - shared, shared)
    heads = [pl.ds(0, tall - 2 * shared), *ending(tall - 2 * shared, shared)]
    lasts = ending(tall - shared, shared)
    sent = [
        to_peer(pu.at[at_core(peer, rows, at * lanes, lanes), :], sum_u.at[span, :], send_sem.at[0], part_sem.at[at])
        for at, span in enumerate(spans_u)
    ]
    for at, span in enumerate(heads):
        sent.append(to_peer(pd.at[span, columns(peer)], sum_d.at[span, :], send_sem.at[0], part_sem.at[groups + at]))

    @pl.when(me == 0)
    def _():
        for at, span in enumerate(lasts):
            to_peer(pd.at[span, columns(peer)], sum_d.at[span, :], send_sem.at[0], part_sem.at[groups + 3 + at])
        for at, span in enumerate(lasts):
            to_peer(pd.at[span, columns(me)], other_d.at[0, span, :], send_sem.at[0], part_sem.at[groups + 5 + at])

    load(md_h, md, load_sem.at[1])
    load(ed_h, ed, load_sem.at[1])
    load(eu_h, eu, load_sem.at[1])
    load(pd.at[:, columns(me)], own_d, load_sem.at[1])

    wait_for(other_d, load_sem.at[0])
    load(pd.at[:, columns(peer)], give_d, load_sem.at[0])
    for copy in small:
        copy.wait()
    load(pu.at[at_core(peer, rows, first, rows - first), :], give_u, small_sem.at[0])

    @blocks(rows, step_u)
    def _(at):
        span = pl.ds(at, step_u)
        x = mu[span, :]
        sq_u[span, :] = lane_sums(x * x)

    def store_size(group, which):
        size = jnp.sum(sq_u[spans_u[group], :].T, axis=0).reshape(1, 1, lanes)
        if group < gathered:
            stat_u[pl.ds(group * n + here, 1), which : which + 1, :] = size
        else:
            at = (2 * (group - gathered) + me) * n + here
            stat_w[pl.ds(at, 1), which : which + 1, :] = size

    for group in range(groups):
        store_size(group, 0)

    def sizes(ref, at, send, recv, cores):
        for step in (*range(1, n), 0):
            for core in range(cores):
                if step + core > 0:
                    target = me if cores == 1 else core if step else peer
                    pltpu.make_async_remote_copy(
                        src_ref=ref.at[at],
                        dst_ref=ref.at[at],
                        send_sem=small_sem.at[send],
                        recv_sem=recv,
                        device_id={"dp": target, "tp": lax.rem(here + step, n)},
                    ).start()

    def sum_rows(group):
        sent[group].wait_recv()

        @blocks(lanes, step_u)
        def _(at):
            span = pl.ds(pl.multiple_of(group * lanes + at, step_u), step_u)
            x = own_u[span, :] + sum_u[span, :]
            sum_u[span, :] = x
            sq_u[span, :] = lane_sums(x * x)

        store_size(group, 1)

    def send_sizes(group):
        if group < gathered:
            sizes(stat_u, group * n + here, 1, stat_sem.at[group], 1)
        else:
            sizes(stat_w, (2 * (group - gathered) + me) * n + here, 2, stat_sem.at[group], 2)

    def meet():
        @pl.when(me == 1)
        def _():
            pl.semaphore_wait(barrier, n - 1)
            pl.semaphore_signal(ready, inc=1, device_id={"dp": peer})

        @pl.when(me == 0)
        def _():
            pl.semaphore_wait(ready, 1)

    for group in range(groups - 1):
        sum_rows(group)

        @pl.when(2 * here >= n)
        def _(group=group):
            if group == 0:
                meet()
            send_sizes(group)

    half = mn.shape[-1]
    vec[0:1, :] = pn_v[...]
    vec[1:2, :] = pb_v[...]
    vec[2:3, :half] = mn_v[...].reshape(1, half)
    vec[2:3, half:] = en_v[...].reshape(1, half)
    vec[3:4, :half] = mb_v[...].reshape(1, half)
    vec[3:4, half:] = eb_v[...].reshape(1, half)
    send_vec = to_peer(vec, got_vec, small_sem.at[4], more_sem.at[2])

    wait_for(pack.at[pl.ds(0, 4)], load_sem.at[1])
    acc_d[...] = jnp.zeros_like(acc_d)
    acc_o[...] = jnp.zeros_like(acc_o)
    stat_d[pl.ds(me * n + here, 1), 1:2, :] = jnp.zeros((1, 1, cols), jnp.float32)

    def eighths(x):
        return jnp.sum(x.reshape(x.shape[0] // 8, 8, cols), axis=0)

    @blocks(tall, step_d)
    def _(at):
        span = pl.ds(at, step_d)
        x = md[span, :]
        base_d[span, :] = x - (learn_rate * hold_rate) * ed[span, :]
        acc_d[...] += eighths(x * x)

    slot_d = me * n + here
    stat_m[pl.ds(slot_d, 1), :, :] = jnp.sum(acc_d[...], axis=0).reshape(1, 1, cols)
    acc_d[...] = jnp.zeros_like(acc_d)

    @blocks(rows - first, step_u)
    def _(at):
        span = pl.ds(pl.multiple_of(first + at, step_u), step_u)
        base_u[pl.ds(at, step_u), :] = mu[span, :] - (learn_rate * hold_rate) * eu[span, :]

    to_peer(own_u.at[rest, :], other_u.at[0], send_sem.at[0], more_sem.at[0])
    to_peer(base_u, other_u.at[1], send_sem.at[0], more_sem.at[0])

    @pl.when(me == 0)
    def _():
        to_peer(own_d.at[head, :], other_d.at[0, head, :], send_sem.at[0], more_sem.at[1])

    @pl.when(me == 1)
    def _():
        to_peer(own_d, other_d.at[0], send_sem.at[0], more_sem.at[1])
        to_peer(pd.at[last, columns(peer)], sum_d.at[last, :], send_sem.at[0], part_sem.at[groups + 3])

    to_peer(base_d, other_d.at[1], send_sem.at[0], more_sem.at[4])

    @pl.when(2 * here < n)
    def _():
        meet()
        for group in range(groups - 1):
            send_sizes(group)

    sum_rows(groups - 1)
    send_sizes(groups - 1)
    sizes(stat_m, slot_d, 5, stat_sem.at[groups + 1], 2)

    def sum_columns(part, acc, one, two, total=None):
        step = step_d if part.size % step_d == 0 else 32

        @blocks(part.size, step)
        def _(at):
            span = pl.ds(pl.multiple_of(part.start + at, 32), step)
            x = one[span, :] + two[span, :]
            if total is not None:
                total[span, :] = x
            if acc is not None:
                acc[...] += eighths(x * x)

    wait_for(give_d, load_sem.at[0])
    for at, span in enumerate(heads):
        sent[groups + at].wait_recv()
        sum_columns(span, acc_d, own_d, sum_d, sum_d)

    def store_total(acc, which):
        stat_d[pl.ds(slot_d, 1), which : which + 1, :] = jnp.sum(acc[...], axis=0).reshape(1, 1, cols)

    @pl.when(me == 0)
    def _():
        store_total(acc_d, 0)

    @pl.when(me == 1)
    def _():
        for at, span in enumerate(lasts):
            wait_for(sum_d.at[span, :], part_sem.at[groups + 3 + at])
            sum_columns(span, acc_d, own_d, sum_d, sum_d)
        store_total(acc_d, 0)
        for at, span in enumerate(lasts):
            wait_for(sum_d.at[span, :], part_sem.at[groups + 5 + at])
            sum_columns(span, acc_o, give_d, other_d.at[0])
        store_total(acc_o, 1)

    sizes(stat_d, slot_d, 3, stat_sem.at[groups], 2)

    for group in range(groups):
        span = spans_u[group]
        if group < gathered:
            wait_for(stat_u.at[pl.ds(0, n - 1)], stat_sem.at[group])
            sq_u[span, :] = jnp.broadcast_to(scale_at(stat_u, group * n, n, rate), (lanes, lanes)).T
        else:
            wait_for(stat_w.at[pl.ds(0, 2 * n - 1)], stat_sem.at[group])
            at = 2 * (group - gathered)
            sq_u[span, :] = jnp.broadcast_to(scale_at(stat_w, (at + me) * n, n, rate), (lanes, lanes)).T
            sq_o[pl.ds((group - gathered) * lanes, lanes), :] = jnp.broadcast_to(
                scale_at(stat_w, (at + peer) * n, n, rate), (lanes, lanes)
            ).T
        if group < gathered:

            @blocks(lanes, step_u)
            def _(at):
                start = pl.multiple_of(group * lanes + at, step_u)
                span = pl.ds(start, step_u)
                scale = jnp.concatenate([sq_u[span, :]] * (wide // lanes), axis=1)
                state = hold_rate * eu[span, :] + sum_u[span, :] * scale
                stepped = mu[span, :] - learn_rate * state
                tu[span, :] = state
                su[span, :] = stepped
                cu[pl.ds(pl.multiple_of(me * rows + start, step_u), step_u), :] = stepped.astype(cu.dtype)

            part = cu.at[at_core(me, rows, group * lanes, lanes), :]
            to_peer(part, part, send_sem.at[0], more_sem.at[3])
        else:
            if group == gathered:
                wait_for(other_u, more_sem.at[0])
                wait_for(give_u, small_sem.at[0])

            @blocks(lanes, step_u // 2)
            def _(at):
                inner = pl.multiple_of((group - gathered) * lanes + at, step_u // 2)
                start = pl.multiple_of(group * lanes + at, step_u // 2)
                near, span = pl.ds(inner, step_u // 2), pl.ds(start, step_u // 2)
                scale = jnp.concatenate([sq_u[span, :]] * (wide // lanes), axis=1)
                step = sum_u[span, :] * scale
                tu[span, :] = hold_rate * eu[span, :] + step
                stepped = base_u[near, :] - learn_rate * step
                su[span, :] = stepped
                place = pl.ds(pl.multiple_of(me * rows + start, step_u // 2), step_u // 2)
                cu[place, :] = stepped.astype(cu.dtype)
                scale = jnp.concatenate([sq_o[near, :]] * (wide // lanes), axis=1)
                step = (give_u[near, :] + other_u[0, near, :]) * scale
                stepped = other_u[1, near, :] - learn_rate * step
                place = pl.ds(pl.multiple_of(peer * rows + start, step_u // 2), step_u // 2)
                cu[place, :] = stepped.astype(cu.dtype)

    send_vec.wait_recv()
    mean = (vec[0:2, :] + got_vec[0:2, :]) * rate
    for at, (state, stepped, rounded) in enumerate(((tn, sn, cn), (tb, sb, cb))):
        row = slice(2 + at, 3 + at)
        low, high = mean[at : at + 1, :half], mean[at : at + 1, half:]
        new_own = hold_rate * vec[row, half:] + jnp.where(me == 0, low, high)
        own = vec[row, :half] - learn_rate * new_own
        new_other = hold_rate * got_vec[row, half:] + jnp.where(me == 0, high, low)
        other = got_vec[row, :half] - learn_rate * new_other
        state[...] = new_own.reshape(state.shape)
        stepped[...] = own.reshape(stepped.shape)
        whole = jnp.concatenate(
            [jnp.where(me == 0, own, other), jnp.where(me == 0, other, own)], axis=1
        )
        rounded[...] = whole.reshape(rounded.shape).astype(rounded.dtype)

    @pl.when(me == 0)
    def _():
        wait_for(sum_d.at[last, :], part_sem.at[groups + 3])
        sum_columns(last, None, own_d, sum_d, sum_d)
        wait_for(pack.at[0], more_sem.at[1])

    @pl.when(me == 1)
    def _():
        wait_for(pack.at[0, head, :], more_sem.at[1])

    wait_for(base_d, more_sem.at[4])

    send_vec.wait_send()
    wait_for(stat_u.at[pl.ds(0, gathered * (n - 1))], small_sem.at[1])
    wait_for(stat_w.at[pl.ds(0, (groups - gathered) * (2 * n - 1))], small_sem.at[2])
    wait_for(stat_d.at[pl.ds(0, 2 * n - 1)], small_sem.at[3])
    wait_for(stat_m.at[pl.ds(0, 2 * n - 1)], small_sem.at[5])
    wait_for(stat_m.at[pl.ds(0, 2 * n - 1)], stat_sem.at[groups + 1])
    wait_for(stat_d.at[pl.ds(0, 2 * n - 1)], stat_sem.at[groups])
    wait_for(cu.at[at_core(peer, rows, 0, first), :], more_sem.at[3])
    wait_for(pack, send_sem.at[0])


def finish(
    cu_v, cn_v, cb_v, su_v, sn_v, sb_v, tu_v, tn_v, tb_v,
    pack, ed, stat_d, stat_m,
    cu, cd, cn, cb, su, sd, sn, sb, tu, td, tn, tb,
    cd_v, sd_v, td_v,
):
    me = lax.axis_index("dp")
    rate = lax.axis_size("dp") ** (-0.5)
    n = lax.axis_size("tp")
    tall, cols = td_v.shape
    step = 32
    mine_d, base_o, sum_d, base_d, give_d = (pack.at[at] for at in range(5))

    def out(source, target, sem):
        copy = pltpu.make_async_copy(source, target, sem)
        copy.start()
        return copy

    def write(sem):
        small = [
            pltpu.make_async_copy(source, target, sem.at[2 + at])
            for at, (source, target) in enumerate(
                ((cn_v, cn), (cb_v, cb), (sn_v, sn), (sb_v, sb), (tn_v, tn), (tb_v, tb))
            )
        ]
        for copy in small:
            copy.start()
        matrices(sem)
        for copy in small:
            copy.wait()
        wait_for(cu_v, sem.at[1])
        wait_for(pack, sem.at[0])

    def matrices(sem):
        out(su_v, su, sem.at[0])
        out(tu_v, tu, sem.at[0])
        out(cu_v, cu, sem.at[1])

        scales = []
        for core in (me, 1 - me):
            weights = sizes = 0.0
            for at in range(n):
                near, far = stat_d[core * n + at], stat_d[(1 - core) * n + at]
                weights = weights + stat_m[core * n + at]
                sizes = sizes + near[0:1, :] + far[1:2, :]
            scales.append(scale_of(weights, sizes, rate))
        own, other = scales
        for piece in range(pieces):
            size = tall // pieces

            @blocks(size, step)
            def _(at):
                span = pl.ds(pl.multiple_of(piece * size + at, step), step)
                x = sum_d[span, :] * own
                td_v[span, :] = hold_rate * ed[span, :] + x
                stepped = base_d[span, :] - learn_rate * x
                sd_v[span, :] = stepped
                cd_v[span, pl.ds(pl.multiple_of(me * cols, cols), cols)] = stepped.astype(cd_v.dtype)
                x = (give_d[span, :] + mine_d[span, :]) * other
                stepped = base_o[span, :] - learn_rate * x
                cd_v[span, pl.ds(pl.multiple_of((1 - me) * cols, cols), cols)] = stepped.astype(cd_v.dtype)

            span = pl.ds(piece * size, size)
            out(td_v.at[span, :], td.at[span, :], sem.at[0])
            out(sd_v.at[span, :], sd.at[span, :], sem.at[0])
            out(cd_v.at[span, :], cd.at[span, :], sem.at[0])

    pl.run_scoped(write, pltpu.SemaphoreType.DMA((8,)))


def held(arrays):
    return [pltpu.with_memory_space_constraint(x, pltpu.HBM) for x in arrays]


def on_pair(*args):
    pu, pd, pn, pb, mu, md, mn, mb, eu, ed, en, eb = args
    n = lax.axis_size("tp")
    f32, bf16 = jnp.float32, jnp.bfloat16
    vmem = pl.BlockSpec(memory_space=pltpu.VMEM)
    hbm = pl.BlockSpec(memory_space=pltpu.HBM)
    wide, tall = pu.shape[2], pd.shape[1]
    rows, cols = mu.shape[0], md.shape[1]
    groups = rows // lanes
    rest = rows - gathered * lanes

    def shaped(shape, dtype=f32):
        return jax.ShapeDtypeStruct(shape, dtype)

    between = [
        shaped((pu.shape[1], wide), bf16), shaped((pn.shape[1],), bf16), shaped((pb.shape[1],), bf16),
        *(shaped(x.shape) for x in (mu, mn, mb)),
        *(shaped(x.shape) for x in (mu, mn, mb)),
        shaped((5, *md.shape)),
        shaped(md.shape),
        shaped((2 * n, 2, cols)),
        shaped((2 * n, 1, cols)),
    ]
    results = pl.pallas_call(
        exchange,
        out_shape=between,
        in_specs=[hbm] * len(args),
        out_specs=[vmem] * len(between),
        scratch_shapes=[
            pltpu.VMEM(mu.shape, f32),
            pltpu.VMEM(md.shape, f32),
            pltpu.VMEM((rest, wide), f32),
            pltpu.VMEM(mu.shape, f32),
            pltpu.VMEM((rest, wide), f32),
            pltpu.VMEM((2, rest, wide), f32),
            *(pltpu.VMEM(x.shape, f32) for x in (mu, md, mu)),
            *(pltpu.VMEM(x.shape, f32) for x in (pn, pb, mn, mb, en, eb)),
            pltpu.VMEM((4, pn.shape[1]), f32),
            pltpu.VMEM((4, pn.shape[1]), f32),
            pltpu.VMEM((rows, lanes), f32),
            pltpu.VMEM((rest, lanes), f32),
            pltpu.VMEM((8, cols), f32),
            pltpu.VMEM((8, cols), f32),
            pltpu.VMEM((gathered * n, 2, lanes), f32),
            pltpu.VMEM(((groups - gathered) * 2 * n, 2, lanes), f32),
        ],
        compiler_params=pltpu.CompilerParams(
            collective_id=0, has_side_effects=True, vmem_limit_bytes=40 * 2**20
        ),
        name="exchange",
    )(*held((pu[0], pd[0], *args[2:])))
    outs = (
        ((pu.shape[1], wide), bf16),
        ((tall, pd.shape[2]), bf16),
        ((pn.shape[1],), bf16),
        ((pb.shape[1],), bf16),
        *((x.shape, f32) for x in (mu, md, mn, mb)),
        *((x.shape, f32) for x in (mu, md, mn, mb)),
    )
    return tuple(pl.pallas_call(
        finish,
        out_shape=[shaped(shape, dtype) for shape, dtype in outs],
        in_specs=[vmem] * len(between),
        out_specs=[hbm] * len(outs),
        scratch_shapes=[
            pltpu.VMEM((tall, pd.shape[2]), bf16),
            pltpu.VMEM(md.shape, f32),
            pltpu.VMEM(md.shape, f32),
        ],
        compiler_params=pltpu.CompilerParams(vmem_limit_bytes=8 * 2**20),
        name="finish",
    )(*results))


def solution(mesh):
    in_specs = (
        P(("job", "dp"), None, "tp"),
        P(("job", "dp"), "tp", None),
        P(("job", "dp"), None),
        P(("job", "dp"), None),
        P(("job", "dp"), "tp"),
        P(("job", "tp"), "dp"),
        P(("job", "dp")),
        P(("job", "dp")),
        P(("job", "dp"), "tp"),
        P(("job", "tp"), "dp"),
        P(("job", "dp")),
        P(("job", "dp")),
    )
    out_specs = (
        P("job", "tp"),
        P(("job", "tp"), None),
        P("job"),
        P("job"),
        P(("job", "dp"), "tp"),
        P(("job", "tp"), "dp"),
        P(("job", "dp")),
        P(("job", "dp")),
        P(("job", "dp"), "tp"),
        P(("job", "tp"), "dp"),
        P(("job", "dp")),
        P(("job", "dp")),
    )
    return jax.shard_map(
        on_device if mesh.shape["dp"] != 2 else on_pair, mesh=mesh, in_specs=in_specs, out_specs=out_specs, check_vma=False
    )
```

```python
import functools

import jax
import jax.numpy as jnp
from jax import lax
from jax.experimental import pallas as pl
from jax.experimental.pallas import tpu as pltpu
from jax.sharding import PartitionSpec as P

learn_rate = 0.4
hold_rate = 0.9


def on_device(
    partial_up,
    partial_down,
    partial_norm,
    partial_bias,
    master_up,
    master_down,
    master_norm,
    master_bias,
    memory_up,
    memory_down,
    memory_norm,
    memory_bias,
):
    mean_up, mean_down = (
        lax.psum_scatter(partial_up[0], "dp", scatter_dimension=0, tiled=True),
        lax.psum_scatter(partial_down[0], "dp", scatter_dimension=1, tiled=True),
    )
    whole_norm, whole_bias = lax.psum((partial_norm[0], partial_bias[0]), "dp")
    place = lax.axis_index("dp")
    mean_norm = lax.dynamic_slice_in_dim(
        whole_norm, place * master_norm.shape[0], master_norm.shape[0]
    )
    mean_bias = lax.dynamic_slice_in_dim(
        whole_bias, place * master_bias.shape[0], master_bias.shape[0]
    )
    mean_rate = lax.axis_size("dp") ** (-0.5)
    mean_up = mean_up * mean_rate
    mean_down = mean_down * mean_rate
    mean_norm = mean_norm * mean_rate
    mean_bias = mean_bias * mean_rate
    own_up, own_down, slope_up_norm, slope_down_norm = lax.psum(
        (
            jnp.sum(master_up * master_up, axis=1, keepdims=True),
            jnp.sum(master_down * master_down, axis=0, keepdims=True),
            jnp.sum(mean_up * mean_up, axis=1, keepdims=True),
            jnp.sum(mean_down * mean_down, axis=0, keepdims=True),
        ),
        "tp",
    )
    mean_up = mean_up * (jnp.sqrt(own_up) * lax.rsqrt(slope_up_norm + 1e-06))
    mean_down = mean_down * (jnp.sqrt(own_down) * lax.rsqrt(slope_down_norm + 1e-06))
    state_new_up = hold_rate * memory_up + mean_up
    stepped_up = master_up - learn_rate * state_new_up
    state_new_down = hold_rate * memory_down + mean_down
    stepped_down = master_down - learn_rate * state_new_down
    state_new_norm = hold_rate * memory_norm + mean_norm
    stepped_norm = master_norm - learn_rate * state_new_norm
    state_new_bias = hold_rate * memory_bias + mean_bias
    stepped_bias = master_bias - learn_rate * state_new_bias
    compute_up, compute_down, compute_norm, compute_bias = (
        lax.all_gather(stepped_up.astype(jnp.bfloat16), "dp", axis=0, tiled=True),
        lax.all_gather(stepped_down.astype(jnp.bfloat16), "dp", axis=1, tiled=True),
        lax.all_gather(stepped_norm.astype(jnp.bfloat16), "dp", axis=0, tiled=True),
        lax.all_gather(stepped_bias.astype(jnp.bfloat16), "dp", axis=0, tiled=True),
    )
    return (
        compute_up,
        compute_down,
        compute_norm,
        compute_bias,
        stepped_up,
        stepped_down,
        stepped_norm,
        stepped_bias,
        state_new_up,
        state_new_down,
        state_new_norm,
        state_new_bias,
    )


pieces = 4
lanes = 128
gathered = 2


def lane_sums(x):
    total = x[:, :lanes]
    for at in range(lanes, x.shape[1], lanes):
        total = total + x[:, at : at + lanes]
    return total


def blocks(count, step):
    def over(body):
        @pl.loop(0, count // step)
        def _(at):
            body(pl.multiple_of(at * step, step))

    return over


def wait_for(ref, sem):
    pltpu.make_async_copy(ref, ref, sem).wait()


def scale_of(weights, sizes, rate):
    return jnp.sqrt(weights) * (lax.rsqrt(sizes * (rate * rate) + 1e-06) * rate)


def scale_at(stat, first, n, rate):
    total = stat[first]
    for at in range(1, n):
        total = total + stat[first + at]
    return scale_of(total[0:1, :], total[1:2, :], rate)


def exchange(*refs):
    groups = refs[4].shape[0] // lanes
    dma, regular = pltpu.SemaphoreType.DMA, pltpu.SemaphoreType.REGULAR
    pl.run_scoped(
        functools.partial(exchange_in_scope, *refs),
        dma((2,)), dma((7,)), dma((groups + 7,)), dma((1,)), dma((groups + 3,)), dma((5,)), regular, regular,
    )


def exchange_in_scope(
    pu, pd, pn, pb, mu_h, md_h, mn, mb, eu_h, ed_h, en, eb,
    cu, cn, cb, su, sn, sb, tu, tn, tb,
    pack, ed, stat_d, stat_m, stat_o,
    own_u, own_d, give_u, sum_u, base_u, other_u, mu, md, eu,
    pn_v, pb_v, mn_v, mb_v, en_v, eb_v, vec, got_vec,
    sq_u, sq_o, acc_d, acc_o, stat_u, stat_w,
    load_sem, small_sem, part_sem, send_sem, stat_sem, more_sem, hello, ready,
):
    me = lax.axis_index("dp")
    peer = 1 - me
    here = lax.axis_index("tp")
    n = lax.axis_size("tp")
    rate = lax.axis_size("dp") ** (-0.5)
    rows, wide = mu.shape
    tall, cols = md.shape
    groups = rows // lanes
    step_u, step_d = 32, 64
    shared = 5 * tall // 24 // 32 * 32
    other_d, (sum_d, base_d, give_d) = pack.at[pl.ds(0, 2)], (pack.at[at] for at in range(2, 5))
    first = gathered * lanes
    rest = pl.ds(first, rows - first)

    def at_core(core, size, start=0, count=None):
        return pl.ds(pl.multiple_of(core * size + start, 8), size if count is None else count)

    def columns(core):
        return pl.ds(pl.multiple_of(core * cols, cols), cols)

    def load(source, target, sem):
        copy = pltpu.make_async_copy(source, target, sem)
        copy.start()
        return copy

    barrier = pltpu.get_barrier_semaphore()

    @pl.when(me == 1)
    def _():
        pl.semaphore_signal(barrier, inc=1, device_id={"dp": peer})

    @pl.when(me == 0)
    def _():
        pl.semaphore_wait(barrier, 1)
        pl.semaphore_signal(hello, inc=1, device_id={"dp": peer})

    small = [
        load(source, target, small_sem.at[at])
        for at, (source, target) in enumerate(
            ((pn, pn_v), (pb, pb_v), (mn, mn_v), (mb, mb_v), (en, en_v), (eb, eb_v))
        )
    ]
    load(pu.at[at_core(me, rows), :], own_u, load_sem.at[0])
    load(mu_h, mu, load_sem.at[0])

    @pl.when(me == 1)
    def _():
        pl.semaphore_wait(hello, 1)
        for step in range(1, n):
            pl.semaphore_signal(barrier, inc=1, device_id={"tp": lax.rem(here + step, n)})

    def to_peer(source, target, send, recv):
        copy = pltpu.make_async_remote_copy(
            src_ref=source, dst_ref=target, send_sem=send, recv_sem=recv, device_id={"dp": peer}
        )
        copy.start()
        return copy

    def ending(start, size):
        return [pl.ds(start, size - step_u), pl.ds(start + size - step_u, step_u)]

    spans_u = [pl.ds(at * lanes, lanes) for at in range(groups)]
    head, last = pl.ds(0, tall - shared), pl.ds(tall - shared, shared)
    heads = [pl.ds(0, tall - 2 * shared), *ending(tall - 2 * shared, shared)]
    lasts = ending(tall - shared, shared)
    sent = [
        to_peer(pu.at[at_core(peer, rows, at * lanes, lanes), :], sum_u.at[span, :], send_sem.at[0], part_sem.at[at])
        for at, span in enumerate(spans_u)
    ]
    for at, span in enumerate(heads):
        sent.append(to_peer(pd.at[span, columns(peer)], sum_d.at[span, :], send_sem.at[0], part_sem.at[groups + at]))

    @pl.when(me == 0)
    def _():
        for at, span in enumerate(lasts):
            to_peer(pd.at[span, columns(peer)], sum_d.at[span, :], send_sem.at[0], part_sem.at[groups + 3 + at])
        for at, span in enumerate(lasts):
            to_peer(pd.at[span, columns(me)], other_d.at[0, span, :], send_sem.at[0], part_sem.at[groups + 5 + at])

    load(md_h, md, load_sem.at[1])
    load(ed_h, ed, load_sem.at[1])
    load(eu_h, eu, load_sem.at[1])
    load(pd.at[:, columns(me)], own_d, load_sem.at[1])

    wait_for(other_d, load_sem.at[0])
    load(pd.at[:, columns(peer)], give_d, load_sem.at[0])
    for copy in small:
        copy.wait()
    load(pu.at[at_core(peer, rows, first, rows - first), :], give_u, small_sem.at[0])

    @blocks(rows, step_u)
    def _(at):
        span = pl.ds(at, step_u)
        x = mu[span, :]
        sq_u[span, :] = lane_sums(x * x)

    def store_size(group, which):
        size = jnp.sum(sq_u[spans_u[group], :].T, axis=0).reshape(1, 1, lanes)
        if group < gathered:
            stat_u[pl.ds(group * n + here, 1), which : which + 1, :] = size
        else:
            at = (2 * (group - gathered) + me) * n + here
            stat_w[pl.ds(at, 1), which : which + 1, :] = size

    for group in range(groups):
        store_size(group, 0)

    def sizes(ref, at, send, recv, cores):
        for step in (*range(1, n), 0):
            for core in range(cores):
                if step + core > 0:
                    target = me if cores == 1 else core if step else peer
                    pltpu.make_async_remote_copy(
                        src_ref=ref.at[at],
                        dst_ref=ref.at[at],
                        send_sem=small_sem.at[send],
                        recv_sem=recv,
                        device_id={"dp": target, "tp": lax.rem(here + step, n)},
                    ).start()

    def sum_rows(group):
        sent[group].wait_recv()

        @blocks(lanes, step_u)
        def _(at):
            span = pl.ds(pl.multiple_of(group * lanes + at, step_u), step_u)
            x = own_u[span, :] + sum_u[span, :]
            sum_u[span, :] = x
            sq_u[span, :] = lane_sums(x * x)

        store_size(group, 1)

    def send_sizes(group):
        if group < gathered:
            sizes(stat_u, group * n + here, 1, stat_sem.at[group], 1)
        else:
            sizes(stat_w, (2 * (group - gathered) + me) * n + here, 2, stat_sem.at[group], 2)

    def meet():
        @pl.when(me == 1)
        def _():
            pl.semaphore_wait(barrier, n - 1)
            pl.semaphore_signal(ready, inc=1, device_id={"dp": peer})

        @pl.when(me == 0)
        def _():
            pl.semaphore_wait(ready, 1)

    for group in range(groups - 1):
        sum_rows(group)

        @pl.when(2 * here >= n)
        def _(group=group):
            if group == 0:
                meet()
            send_sizes(group)

    half = mn.shape[-1]
    vec[0:1, :] = pn_v[...]
    vec[1:2, :] = pb_v[...]
    vec[2:3, :half] = mn_v[...].reshape(1, half)
    vec[2:3, half:] = en_v[...].reshape(1, half)
    vec[3:4, :half] = mb_v[...].reshape(1, half)
    vec[3:4, half:] = eb_v[...].reshape(1, half)
    send_vec = to_peer(vec, got_vec, small_sem.at[4], more_sem.at[2])

    wait_for(pack.at[pl.ds(0, 4)], load_sem.at[1])
    acc_d[...] = jnp.zeros_like(acc_d)
    acc_o[...] = jnp.zeros_like(acc_o)

    def eighths(x):
        return jnp.sum(x.reshape(x.shape[0] // 8, 8, cols), axis=0)

    @blocks(tall, step_d)
    def _(at):
        span = pl.ds(at, step_d)
        x = md[span, :]
        base_d[span, :] = x - (learn_rate * hold_rate) * ed[span, :]
        acc_d[...] += eighths(x * x)

    slot_d = me * n + here
    stat_m[pl.ds(slot_d, 1), :, :] = jnp.sum(acc_d[...], axis=0).reshape(1, 1, cols)
    acc_d[...] = jnp.zeros_like(acc_d)

    @blocks(rows - first, step_u)
    def _(at):
        span = pl.ds(pl.multiple_of(first + at, step_u), step_u)
        base_u[pl.ds(at, step_u), :] = mu[span, :] - (learn_rate * hold_rate) * eu[span, :]

    to_peer(own_u.at[rest, :], other_u.at[0], send_sem.at[0], more_sem.at[0])
    to_peer(base_u, other_u.at[1], send_sem.at[0], more_sem.at[0])

    @pl.when(me == 0)
    def _():
        to_peer(own_d.at[head, :], other_d.at[0, head, :], send_sem.at[0], more_sem.at[1])

    @pl.when(me == 1)
    def _():
        to_peer(own_d, other_d.at[0], send_sem.at[0], more_sem.at[1])
        to_peer(pd.at[last, columns(peer)], sum_d.at[last, :], send_sem.at[0], part_sem.at[groups + 3])

    to_peer(base_d, other_d.at[1], send_sem.at[0], more_sem.at[4])

    @pl.when(2 * here < n)
    def _():
        meet()
        for group in range(groups - 1):
            send_sizes(group)

    sum_rows(groups - 1)
    send_sizes(groups - 1)
    sizes(stat_m, slot_d, 5, stat_sem.at[groups + 1], 2)

    def sum_columns(part, acc, one, two, total=None):
        step = step_d if part.size % step_d == 0 else 32

        @blocks(part.size, step)
        def _(at):
            span = pl.ds(pl.multiple_of(part.start + at, 32), step)
            x = one[span, :] + two[span, :]
            if total is not None:
                total[span, :] = x
            if acc is not None:
                acc[...] += eighths(x * x)

    wait_for(give_d, load_sem.at[0])
    for at, span in enumerate(heads):
        sent[groups + at].wait_recv()
        sum_columns(span, acc_d, own_d, sum_d, sum_d)

    def send_total():
        stat_d[pl.ds(slot_d, 1), :, :] = jnp.sum(acc_d[...], axis=0).reshape(1, 1, cols)
        sizes(stat_d, slot_d, 3, stat_sem.at[groups], 2)

    @pl.when(me == 0)
    def _():
        send_total()

    @pl.when(me == 1)
    def _():
        for at, span in enumerate(lasts):
            wait_for(sum_d.at[span, :], part_sem.at[groups + 3 + at])
            sum_columns(span, acc_d, own_d, sum_d, sum_d)
        send_total()
        for at, span in enumerate(lasts):
            wait_for(sum_d.at[span, :], part_sem.at[groups + 5 + at])
            sum_columns(span, acc_o, give_d, other_d.at[0])
        stat_o[pl.ds(here, 1), :, :] = jnp.sum(acc_o[...], axis=0).reshape(1, 1, cols)
        sizes(stat_o, here, 6, stat_sem.at[groups + 2], 2)


    for group in range(groups):
        span = spans_u[group]
        if group < gathered:
            wait_for(stat_u.at[pl.ds(0, n - 1)], stat_sem.at[group])
            sq_u[span, :] = jnp.broadcast_to(scale_at(stat_u, group * n, n, rate), (lanes, lanes)).T
        else:
            wait_for(stat_w.at[pl.ds(0, 2 * n - 1)], stat_sem.at[group])
            at = 2 * (group - gathered)
            sq_u[span, :] = jnp.broadcast_to(scale_at(stat_w, (at + me) * n, n, rate), (lanes, lanes)).T
            sq_o[pl.ds((group - gathered) * lanes, lanes), :] = jnp.broadcast_to(
                scale_at(stat_w, (at + peer) * n, n, rate), (lanes, lanes)
            ).T
        if group < gathered:

            @blocks(lanes, step_u)
            def _(at):
                start = pl.multiple_of(group * lanes + at, step_u)
                span = pl.ds(start, step_u)
                scale = jnp.concatenate([sq_u[span, :]] * (wide // lanes), axis=1)
                state = hold_rate * eu[span, :] + sum_u[span, :] * scale
                stepped = mu[span, :] - learn_rate * state
                tu[span, :] = state
                su[span, :] = stepped
                cu[pl.ds(pl.multiple_of(me * rows + start, step_u), step_u), :] = stepped.astype(cu.dtype)

            part = cu.at[at_core(me, rows, group * lanes, lanes), :]
            to_peer(part, part, send_sem.at[0], more_sem.at[3])
        else:
            if group == gathered:
                wait_for(other_u, more_sem.at[0])
                wait_for(give_u, small_sem.at[0])

            @blocks(lanes, step_u // 2)
            def _(at):
                inner = pl.multiple_of((group - gathered) * lanes + at, step_u // 2)
                start = pl.multiple_of(group * lanes + at, step_u // 2)
                near, span = pl.ds(inner, step_u // 2), pl.ds(start, step_u // 2)
                scale = jnp.concatenate([sq_u[span, :]] * (wide // lanes), axis=1)
                step = sum_u[span, :] * scale
                tu[span, :] = hold_rate * eu[span, :] + step
                stepped = base_u[near, :] - learn_rate * step
                su[span, :] = stepped
                place = pl.ds(pl.multiple_of(me * rows + start, step_u // 2), step_u // 2)
                cu[place, :] = stepped.astype(cu.dtype)
                scale = jnp.concatenate([sq_o[near, :]] * (wide // lanes), axis=1)
                step = (give_u[near, :] + other_u[0, near, :]) * scale
                stepped = other_u[1, near, :] - learn_rate * step
                place = pl.ds(pl.multiple_of(peer * rows + start, step_u // 2), step_u // 2)
                cu[place, :] = stepped.astype(cu.dtype)

    send_vec.wait_recv()
    mean = (vec[0:2, :] + got_vec[0:2, :]) * rate
    for at, (state, stepped, rounded) in enumerate(((tn, sn, cn), (tb, sb, cb))):
        row = slice(2 + at, 3 + at)
        low, high = mean[at : at + 1, :half], mean[at : at + 1, half:]
        new_own = hold_rate * vec[row, half:] + jnp.where(me == 0, low, high)
        own = vec[row, :half] - learn_rate * new_own
        new_other = hold_rate * got_vec[row, half:] + jnp.where(me == 0, high, low)
        other = got_vec[row, :half] - learn_rate * new_other
        state[...] = new_own.reshape(state.shape)
        stepped[...] = own.reshape(stepped.shape)
        whole = jnp.concatenate(
            [jnp.where(me == 0, own, other), jnp.where(me == 0, other, own)], axis=1
        )
        rounded[...] = whole.reshape(rounded.shape).astype(rounded.dtype)

    @pl.when(me == 0)
    def _():
        wait_for(sum_d.at[last, :], part_sem.at[groups + 3])
        sum_columns(last, None, own_d, sum_d, sum_d)
        wait_for(pack.at[0], more_sem.at[1])

    @pl.when(me == 1)
    def _():
        wait_for(pack.at[0, head, :], more_sem.at[1])

    wait_for(base_d, more_sem.at[4])

    send_vec.wait_send()
    wait_for(stat_u.at[pl.ds(0, gathered * (n - 1))], small_sem.at[1])
    wait_for(stat_w.at[pl.ds(0, (groups - gathered) * (2 * n - 1))], small_sem.at[2])
    wait_for(stat_d.at[pl.ds(0, 2 * n - 1)], small_sem.at[3])
    wait_for(stat_m.at[pl.ds(0, 2 * n - 1)], small_sem.at[5])
    wait_for(stat_m.at[pl.ds(0, 2 * n - 1)], stat_sem.at[groups + 1])
    wait_for(stat_d.at[pl.ds(0, 2 * n - 1)], stat_sem.at[groups])

    @pl.when(me == 0)
    def _():
        wait_for(stat_o, stat_sem.at[groups + 2])

    @pl.when(me == 1)
    def _():
        wait_for(stat_o.at[pl.ds(0, n - 1)], stat_sem.at[groups + 2])
        wait_for(stat_d.at[pl.ds(0, 2 * n - 1)], small_sem.at[6])

    wait_for(cu.at[at_core(peer, rows, 0, first), :], more_sem.at[3])
    wait_for(pack, send_sem.at[0])


def finish(
    cu_v, cn_v, cb_v, su_v, sn_v, sb_v, tu_v, tn_v, tb_v,
    pack, ed, stat_d, stat_m, stat_o,
    cu, cd, cn, cb, su, sd, sn, sb, tu, td, tn, tb,
    cd_v, sd_v, td_v,
):
    me = lax.axis_index("dp")
    rate = lax.axis_size("dp") ** (-0.5)
    n = lax.axis_size("tp")
    tall, cols = td_v.shape
    step = 32
    mine_d, base_o, sum_d, base_d, give_d = (pack.at[at] for at in range(5))

    def out(source, target, sem):
        copy = pltpu.make_async_copy(source, target, sem)
        copy.start()
        return copy

    def write(sem):
        small = [
            pltpu.make_async_copy(source, target, sem.at[2 + at])
            for at, (source, target) in enumerate(
                ((cn_v, cn), (cb_v, cb), (sn_v, sn), (sb_v, sb), (tn_v, tn), (tb_v, tb))
            )
        ]
        for copy in small:
            copy.start()
        matrices(sem)
        for copy in small:
            copy.wait()
        wait_for(cu_v, sem.at[1])
        wait_for(pack, sem.at[0])

    def matrices(sem):
        out(su_v, su, sem.at[0])
        out(tu_v, tu, sem.at[0])
        out(cu_v, cu, sem.at[1])

        scales = []
        for core in (me, 1 - me):
            weights = sizes = 0.0
            for at in range(n):
                weights = weights + stat_m[core * n + at]
                sizes = sizes + stat_d[core * n + at] + jnp.where(core == 0, stat_o[at], 0.0)
            scales.append(scale_of(weights, sizes, rate))
        own, other = scales
        for piece in range(pieces):
            size = tall // pieces

            @blocks(size, step)
            def _(at):
                span = pl.ds(pl.multiple_of(piece * size + at, step), step)
                x = sum_d[span, :] * own
                td_v[span, :] = hold_rate * ed[span, :] + x
                stepped = base_d[span, :] - learn_rate * x
                sd_v[span, :] = stepped
                cd_v[span, pl.ds(pl.multiple_of(me * cols, cols), cols)] = stepped.astype(cd_v.dtype)
                x = (give_d[span, :] + mine_d[span, :]) * other
                stepped = base_o[span, :] - learn_rate * x
                cd_v[span, pl.ds(pl.multiple_of((1 - me) * cols, cols), cols)] = stepped.astype(cd_v.dtype)

            span = pl.ds(piece * size, size)
            out(td_v.at[span, :], td.at[span, :], sem.at[0])
            out(sd_v.at[span, :], sd.at[span, :], sem.at[0])
            out(cd_v.at[span, :], cd.at[span, :], sem.at[0])

    pl.run_scoped(write, pltpu.SemaphoreType.DMA((8,)))


def held(arrays):
    return [pltpu.with_memory_space_constraint(x, pltpu.HBM) for x in arrays]


def on_pair(*args):
    pu, pd, pn, pb, mu, md, mn, mb, eu, ed, en, eb = args
    n = lax.axis_size("tp")
    f32, bf16 = jnp.float32, jnp.bfloat16
    vmem = pl.BlockSpec(memory_space=pltpu.VMEM)
    hbm = pl.BlockSpec(memory_space=pltpu.HBM)
    wide, tall = pu.shape[2], pd.shape[1]
    rows, cols = mu.shape[0], md.shape[1]
    groups = rows // lanes
    rest = rows - gathered * lanes

    def shaped(shape, dtype=f32):
        return jax.ShapeDtypeStruct(shape, dtype)

    between = [
        shaped((pu.shape[1], wide), bf16), shaped((pn.shape[1],), bf16), shaped((pb.shape[1],), bf16),
        *(shaped(x.shape) for x in (mu, mn, mb)),
        *(shaped(x.shape) for x in (mu, mn, mb)),
        shaped((5, *md.shape)),
        shaped(md.shape),
        shaped((2 * n, 1, cols)),
        shaped((2 * n, 1, cols)),
        shaped((n, 1, cols)),
    ]
    results = pl.pallas_call(
        exchange,
        out_shape=between,
        in_specs=[hbm] * len(args),
        out_specs=[vmem] * len(between),
        scratch_shapes=[
            pltpu.VMEM(mu.shape, f32),
            pltpu.VMEM(md.shape, f32),
            pltpu.VMEM((rest, wide), f32),
            pltpu.VMEM(mu.shape, f32),
            pltpu.VMEM((rest, wide), f32),
            pltpu.VMEM((2, rest, wide), f32),
            *(pltpu.VMEM(x.shape, f32) for x in (mu, md, mu)),
            *(pltpu.VMEM(x.shape, f32) for x in (pn, pb, mn, mb, en, eb)),
            pltpu.VMEM((4, pn.shape[1]), f32),
            pltpu.VMEM((4, pn.shape[1]), f32),
            pltpu.VMEM((rows, lanes), f32),
            pltpu.VMEM((rest, lanes), f32),
            pltpu.VMEM((8, cols), f32),
            pltpu.VMEM((8, cols), f32),
            pltpu.VMEM((gathered * n, 2, lanes), f32),
            pltpu.VMEM(((groups - gathered) * 2 * n, 2, lanes), f32),
        ],
        compiler_params=pltpu.CompilerParams(
            collective_id=0, has_side_effects=True, vmem_limit_bytes=40 * 2**20
        ),
        name="exchange",
    )(*held((pu[0], pd[0], *args[2:])))
    outs = (
        ((pu.shape[1], wide), bf16),
        ((tall, pd.shape[2]), bf16),
        ((pn.shape[1],), bf16),
        ((pb.shape[1],), bf16),
        *((x.shape, f32) for x in (mu, md, mn, mb)),
        *((x.shape, f32) for x in (mu, md, mn, mb)),
    )
    return tuple(pl.pallas_call(
        finish,
        out_shape=[shaped(shape, dtype) for shape, dtype in outs],
        in_specs=[vmem] * len(between),
        out_specs=[hbm] * len(outs),
        scratch_shapes=[
            pltpu.VMEM((tall, pd.shape[2]), bf16),
            pltpu.VMEM(md.shape, f32),
            pltpu.VMEM(md.shape, f32),
        ],
        compiler_params=pltpu.CompilerParams(vmem_limit_bytes=8 * 2**20),
        name="finish",
    )(*results))


def solution(mesh):
    in_specs = (
        P(("job", "dp"), None, "tp"),
        P(("job", "dp"), "tp", None),
        P(("job", "dp"), None),
        P(("job", "dp"), None),
        P(("job", "dp"), "tp"),
        P(("job", "tp"), "dp"),
        P(("job", "dp")),
        P(("job", "dp")),
        P(("job", "dp"), "tp"),
        P(("job", "tp"), "dp"),
        P(("job", "dp")),
        P(("job", "dp")),
    )
    out_specs = (
        P("job", "tp"),
        P(("job", "tp"), None),
        P("job"),
        P("job"),
        P(("job", "dp"), "tp"),
        P(("job", "tp"), "dp"),
        P(("job", "dp")),
        P(("job", "dp")),
        P(("job", "dp"), "tp"),
        P(("job", "tp"), "dp"),
        P(("job", "dp")),
        P(("job", "dp")),
    )
    return jax.shard_map(
        on_device if mesh.shape["dp"] != 2 else on_pair, mesh=mesh, in_specs=in_specs, out_specs=out_specs, check_vma=False
    )
```

```python
import functools

import jax
import jax.numpy as jnp
from jax import lax
from jax.experimental import pallas as pl
from jax.experimental.pallas import tpu as pltpu
from jax.sharding import PartitionSpec as P

learn_rate = 0.4
hold_rate = 0.9


def on_device(
    partial_up,
    partial_down,
    partial_norm,
    partial_bias,
    master_up,
    master_down,
    master_norm,
    master_bias,
    memory_up,
    memory_down,
    memory_norm,
    memory_bias,
):
    mean_up, mean_down = (
        lax.psum_scatter(partial_up[0], "dp", scatter_dimension=0, tiled=True),
        lax.psum_scatter(partial_down[0], "dp", scatter_dimension=1, tiled=True),
    )
    whole_norm, whole_bias = lax.psum((partial_norm[0], partial_bias[0]), "dp")
    place = lax.axis_index("dp")
    mean_norm = lax.dynamic_slice_in_dim(
        whole_norm, place * master_norm.shape[0], master_norm.shape[0]
    )
    mean_bias = lax.dynamic_slice_in_dim(
        whole_bias, place * master_bias.shape[0], master_bias.shape[0]
    )
    mean_rate = lax.axis_size("dp") ** (-0.5)
    mean_up = mean_up * mean_rate
    mean_down = mean_down * mean_rate
    mean_norm = mean_norm * mean_rate
    mean_bias = mean_bias * mean_rate
    own_up, own_down, slope_up_norm, slope_down_norm = lax.psum(
        (
            jnp.sum(master_up * master_up, axis=1, keepdims=True),
            jnp.sum(master_down * master_down, axis=0, keepdims=True),
            jnp.sum(mean_up * mean_up, axis=1, keepdims=True),
            jnp.sum(mean_down * mean_down, axis=0, keepdims=True),
        ),
        "tp",
    )
    mean_up = mean_up * (jnp.sqrt(own_up) * lax.rsqrt(slope_up_norm + 1e-06))
    mean_down = mean_down * (jnp.sqrt(own_down) * lax.rsqrt(slope_down_norm + 1e-06))
    state_new_up = hold_rate * memory_up + mean_up
    stepped_up = master_up - learn_rate * state_new_up
    state_new_down = hold_rate * memory_down + mean_down
    stepped_down = master_down - learn_rate * state_new_down
    state_new_norm = hold_rate * memory_norm + mean_norm
    stepped_norm = master_norm - learn_rate * state_new_norm
    state_new_bias = hold_rate * memory_bias + mean_bias
    stepped_bias = master_bias - learn_rate * state_new_bias
    compute_up, compute_down, compute_norm, compute_bias = (
        lax.all_gather(stepped_up.astype(jnp.bfloat16), "dp", axis=0, tiled=True),
        lax.all_gather(stepped_down.astype(jnp.bfloat16), "dp", axis=1, tiled=True),
        lax.all_gather(stepped_norm.astype(jnp.bfloat16), "dp", axis=0, tiled=True),
        lax.all_gather(stepped_bias.astype(jnp.bfloat16), "dp", axis=0, tiled=True),
    )
    return (
        compute_up,
        compute_down,
        compute_norm,
        compute_bias,
        stepped_up,
        stepped_down,
        stepped_norm,
        stepped_bias,
        state_new_up,
        state_new_down,
        state_new_norm,
        state_new_bias,
    )


pieces = 4
lanes = 128
gathered = 2


def lane_sums(x):
    total = x[:, :lanes]
    for at in range(lanes, x.shape[1], lanes):
        total = total + x[:, at : at + lanes]
    return total


def blocks(count, step):
    def over(body):
        @pl.loop(0, count // step)
        def _(at):
            body(pl.multiple_of(at * step, step))

    return over


def wait_for(ref, sem):
    pltpu.make_async_copy(ref, ref, sem).wait()


def scale_of(weights, sizes, rate):
    return jnp.sqrt(weights) * (lax.rsqrt(sizes * (rate * rate) + 1e-06) * rate)


def scale_at(stat, first, n, rate):
    total = stat[first]
    for at in range(1, n):
        total = total + stat[first + at]
    return scale_of(total[0:1, :], total[1:2, :], rate)


def exchange(*refs):
    groups = refs[4].shape[0] // lanes
    dma, regular = pltpu.SemaphoreType.DMA, pltpu.SemaphoreType.REGULAR
    pl.run_scoped(
        functools.partial(exchange_in_scope, *refs),
        dma((2,)), dma((7,)), dma((groups + 7,)), dma((1,)), dma((groups + 3,)), dma((5,)), regular, regular,
    )


def exchange_in_scope(
    pu, pd, pn, pb, mu_h, md_h, mn, mb, eu_h, ed_h, en, eb,
    cu, cn, cb, su, sn, sb, tu, tn, tb,
    pack, ed, stat_d, stat_m, stat_o,
    own_u, own_d, give_u, sum_u, base_u, other_u, mu, md, eu,
    pn_v, pb_v, mn_v, mb_v, en_v, eb_v, vec, got_vec,
    sq_u, sq_o, acc_d, acc_o, stat_u, stat_w,
    load_sem, small_sem, part_sem, send_sem, stat_sem, more_sem, hello, ready,
):
    me = lax.axis_index("dp")
    peer = 1 - me
    here = lax.axis_index("tp")
    n = lax.axis_size("tp")
    rate = lax.axis_size("dp") ** (-0.5)
    rows, wide = mu.shape
    tall, cols = md.shape
    groups = rows // lanes
    step_u, step_d = 32, 64
    shared = 5 * tall // 24 // 32 * 32
    other_d, (sum_d, base_d, give_d) = pack.at[pl.ds(0, 2)], (pack.at[at] for at in range(2, 5))
    first = gathered * lanes
    rest = pl.ds(first, rows - first)

    def at_core(core, size, start=0, count=None):
        return pl.ds(pl.multiple_of(core * size + start, 8), size if count is None else count)

    def columns(core):
        return pl.ds(pl.multiple_of(core * cols, cols), cols)

    def load(source, target, sem):
        copy = pltpu.make_async_copy(source, target, sem)
        copy.start()
        return copy

    barrier = pltpu.get_barrier_semaphore()

    @pl.when(me == 1)
    def _():
        pl.semaphore_signal(barrier, inc=1, device_id={"dp": peer})

    @pl.when(me == 0)
    def _():
        pl.semaphore_wait(barrier, 1)
        pl.semaphore_signal(hello, inc=1, device_id={"dp": peer})

    small = [
        load(source, target, small_sem.at[at])
        for at, (source, target) in enumerate(
            ((pn, pn_v), (pb, pb_v), (mn, mn_v), (mb, mb_v), (en, en_v), (eb, eb_v))
        )
    ]
    load(pu.at[at_core(me, rows), :], own_u, load_sem.at[0])
    load(mu_h, mu, load_sem.at[0])

    @pl.when(me == 1)
    def _():
        pl.semaphore_wait(hello, 1)
        for step in range(1, n):
            pl.semaphore_signal(barrier, inc=1, device_id={"tp": lax.rem(here + step, n)})

    def to_peer(source, target, send, recv):
        copy = pltpu.make_async_remote_copy(
            src_ref=source, dst_ref=target, send_sem=send, recv_sem=recv, device_id={"dp": peer}
        )
        copy.start()
        return copy

    def ending(start, size):
        return [pl.ds(start, size - step_u), pl.ds(start + size - step_u, step_u)]

    spans_u = [pl.ds(at * lanes, lanes) for at in range(groups)]
    head, last = pl.ds(0, tall - shared), pl.ds(tall - shared, shared)
    heads = [pl.ds(0, tall - 2 * shared), *ending(tall - 2 * shared, shared)]
    lasts = ending(tall - shared, shared)
    sent = [
        to_peer(pu.at[at_core(peer, rows, at * lanes, lanes), :], sum_u.at[span, :], send_sem.at[0], part_sem.at[at])
        for at, span in enumerate(spans_u)
    ]
    for at, span in enumerate(heads):
        sent.append(to_peer(pd.at[span, columns(peer)], sum_d.at[span, :], send_sem.at[0], part_sem.at[groups + at]))

    @pl.when(me == 0)
    def _():
        for at, span in enumerate(lasts):
            to_peer(pd.at[span, columns(peer)], sum_d.at[span, :], send_sem.at[0], part_sem.at[groups + 3 + at])
        for at, span in enumerate(lasts):
            to_peer(pd.at[span, columns(me)], other_d.at[0, span, :], send_sem.at[0], part_sem.at[groups + 5 + at])

    load(md_h, md, load_sem.at[1])
    load(ed_h, ed, load_sem.at[1])
    load(eu_h, eu, load_sem.at[1])
    load(pd.at[:, columns(me)], own_d, load_sem.at[1])

    wait_for(other_d, load_sem.at[0])
    load(pd.at[:, columns(peer)], give_d, load_sem.at[0])
    for copy in small:
        copy.wait()
    load(pu.at[at_core(peer, rows, first, rows - first), :], give_u, small_sem.at[0])

    @blocks(rows, step_u)
    def _(at):
        span = pl.ds(at, step_u)
        x = mu[span, :]
        sq_u[span, :] = lane_sums(x * x)

    def store_size(group, which):
        size = jnp.sum(sq_u[spans_u[group], :].T, axis=0).reshape(1, 1, lanes)
        if group < gathered:
            stat_u[pl.ds(group * n + here, 1), which : which + 1, :] = size
        else:
            at = (2 * (group - gathered) + me) * n + here
            stat_w[pl.ds(at, 1), which : which + 1, :] = size

    for group in range(groups):
        store_size(group, 0)

    def sizes(ref, at, send, recv, cores):
        for step in (*range(1, n), 0):
            for core in range(cores):
                if step + core > 0:
                    target = me if cores == 1 else core if step else peer
                    pltpu.make_async_remote_copy(
                        src_ref=ref.at[at],
                        dst_ref=ref.at[at],
                        send_sem=small_sem.at[send],
                        recv_sem=recv,
                        device_id={"dp": target, "tp": lax.rem(here + step, n)},
                    ).start()

    def sum_rows(group):
        sent[group].wait_recv()

        @blocks(lanes, step_u)
        def _(at):
            span = pl.ds(pl.multiple_of(group * lanes + at, step_u), step_u)
            x = own_u[span, :] + sum_u[span, :]
            sum_u[span, :] = x
            sq_u[span, :] = lane_sums(x * x)

        store_size(group, 1)

    def send_sizes(group):
        if group < gathered:
            sizes(stat_u, group * n + here, 1, stat_sem.at[group], 1)
        else:
            sizes(stat_w, (2 * (group - gathered) + me) * n + here, 2, stat_sem.at[group], 2)

    def meet():
        @pl.when(me == 1)
        def _():
            pl.semaphore_wait(barrier, n - 1)
            pl.semaphore_signal(ready, inc=1, device_id={"dp": peer})

        @pl.when(me == 0)
        def _():
            pl.semaphore_wait(ready, 1)

    for group in range(groups - 1):
        sum_rows(group)

        @pl.when(2 * here >= n)
        def _(group=group):
            if group == 0:
                meet()
            send_sizes(group)

    half = mn.shape[-1]
    vec[0:1, :] = pn_v[...]
    vec[1:2, :] = pb_v[...]
    vec[2:3, :half] = mn_v[...].reshape(1, half)
    vec[2:3, half:] = en_v[...].reshape(1, half)
    vec[3:4, :half] = mb_v[...].reshape(1, half)
    vec[3:4, half:] = eb_v[...].reshape(1, half)
    send_vec = to_peer(vec, got_vec, small_sem.at[4], more_sem.at[2])

    wait_for(pack.at[pl.ds(0, 4)], load_sem.at[1])
    acc_d[...] = jnp.zeros_like(acc_d)
    acc_o[...] = jnp.zeros_like(acc_o)

    def eighths(x):
        return jnp.sum(x.reshape(x.shape[0] // 8, 8, cols), axis=0)

    @blocks(tall, step_d)
    def _(at):
        span = pl.ds(at, step_d)
        x = md[span, :]
        base_d[span, :] = x - (learn_rate * hold_rate) * ed[span, :]
        acc_d[...] += eighths(x * x)

    slot_d = me * n + here
    stat_m[pl.ds(slot_d, 1), :, :] = jnp.sum(acc_d[...], axis=0).reshape(1, 1, cols)
    acc_d[...] = jnp.zeros_like(acc_d)

    @blocks(rows - first, step_u)
    def _(at):
        span = pl.ds(pl.multiple_of(first + at, step_u), step_u)
        base_u[pl.ds(at, step_u), :] = mu[span, :] - (learn_rate * hold_rate) * eu[span, :]

    to_peer(own_u.at[rest, :], other_u.at[0], send_sem.at[0], more_sem.at[0])
    to_peer(base_u, other_u.at[1], send_sem.at[0], more_sem.at[0])

    @pl.when(me == 0)
    def _():
        to_peer(own_d.at[head, :], other_d.at[0, head, :], send_sem.at[0], more_sem.at[1])

    @pl.when(me == 1)
    def _():
        to_peer(own_d, other_d.at[0], send_sem.at[0], more_sem.at[1])
        to_peer(pd.at[last, columns(peer)], sum_d.at[last, :], send_sem.at[0], part_sem.at[groups + 3])

    to_peer(base_d, other_d.at[1], send_sem.at[0], more_sem.at[4])

    @pl.when(2 * here < n)
    def _():
        meet()
        for group in range(groups - 1):
            send_sizes(group)

    sum_rows(groups - 1)
    send_sizes(groups - 1)
    sizes(stat_m, slot_d, 5, stat_sem.at[groups + 1], 2)

    def sum_columns(part, acc, one, two, total=None):
        step = step_d if part.size % step_d == 0 else 32

        @blocks(part.size, step)
        def _(at):
            span = pl.ds(pl.multiple_of(part.start + at, 32), step)
            x = one[span, :] + two[span, :]
            if total is not None:
                total[span, :] = x
            if acc is not None:
                acc[...] += eighths(x * x)

    wait_for(give_d, load_sem.at[0])
    for at, span in enumerate(heads):
        sent[groups + at].wait_recv()
        sum_columns(span, acc_d, own_d, sum_d, sum_d)

    def send_total():
        stat_d[pl.ds(slot_d, 1), :, :] = jnp.sum(acc_d[...], axis=0).reshape(1, 1, cols)
        sizes(stat_d, slot_d, 3, stat_sem.at[groups], 2)

    @pl.when(me == 0)
    def _():
        send_total()

    @pl.when(me == 1)
    def _():
        for at, span in enumerate(lasts):
            wait_for(sum_d.at[span, :], part_sem.at[groups + 3 + at])
            sum_columns(span, acc_d, own_d, sum_d, sum_d)
        send_total()
        for at, span in enumerate(lasts):
            wait_for(sum_d.at[span, :], part_sem.at[groups + 5 + at])
            sum_columns(span, acc_o, give_d, other_d.at[0])
        stat_o[pl.ds(here, 1), :, :] = jnp.sum(acc_o[...], axis=0).reshape(1, 1, cols)
        sizes(stat_o, here, 6, stat_sem.at[groups + 2], 2)


    for group in range(groups):
        span = spans_u[group]
        if group < gathered:
            wait_for(stat_u.at[pl.ds(0, n - 1)], stat_sem.at[group])
            sq_u[span, :] = jnp.broadcast_to(scale_at(stat_u, group * n, n, rate), (lanes, lanes)).T
        else:
            wait_for(stat_w.at[pl.ds(0, 2 * n - 1)], stat_sem.at[group])
            at = 2 * (group - gathered)
            sq_u[span, :] = jnp.broadcast_to(scale_at(stat_w, (at + me) * n, n, rate), (lanes, lanes)).T
            sq_o[pl.ds((group - gathered) * lanes, lanes), :] = jnp.broadcast_to(
                scale_at(stat_w, (at + peer) * n, n, rate), (lanes, lanes)
            ).T
        if group < gathered:

            @blocks(lanes, step_u)
            def _(at):
                start = pl.multiple_of(group * lanes + at, step_u)
                span = pl.ds(start, step_u)
                scale = jnp.concatenate([sq_u[span, :]] * (wide // lanes), axis=1)
                state = hold_rate * eu[span, :] + sum_u[span, :] * scale
                stepped = mu[span, :] - learn_rate * state
                tu[span, :] = state
                su[span, :] = stepped
                cu[pl.ds(pl.multiple_of(me * rows + start, step_u), step_u), :] = stepped.astype(cu.dtype)

            part = cu.at[at_core(me, rows, group * lanes, lanes), :]
            to_peer(part, part, send_sem.at[0], more_sem.at[3])
        else:
            if group == gathered:
                wait_for(other_u, more_sem.at[0])
                wait_for(give_u, small_sem.at[0])

            @blocks(lanes, step_u // 2)
            def _(at):
                inner = pl.multiple_of((group - gathered) * lanes + at, step_u // 2)
                start = pl.multiple_of(group * lanes + at, step_u // 2)
                near, span = pl.ds(inner, step_u // 2), pl.ds(start, step_u // 2)
                scale = jnp.concatenate([sq_u[span, :]] * (wide // lanes), axis=1)
                step = sum_u[span, :] * scale
                tu[span, :] = hold_rate * eu[span, :] + step
                stepped = base_u[near, :] - learn_rate * step
                su[span, :] = stepped
                place = pl.ds(pl.multiple_of(me * rows + start, step_u // 2), step_u // 2)
                cu[place, :] = stepped.astype(cu.dtype)
                scale = jnp.concatenate([sq_o[near, :]] * (wide // lanes), axis=1)
                step = (give_u[near, :] + other_u[0, near, :]) * scale
                stepped = other_u[1, near, :] - learn_rate * step
                place = pl.ds(pl.multiple_of(peer * rows + start, step_u // 2), step_u // 2)
                cu[place, :] = stepped.astype(cu.dtype)

    send_vec.wait_recv()
    mean = (vec[0:2, :] + got_vec[0:2, :]) * rate
    for at, (state, stepped, rounded) in enumerate(((tn, sn, cn), (tb, sb, cb))):
        row = slice(2 + at, 3 + at)
        low, high = mean[at : at + 1, :half], mean[at : at + 1, half:]
        new_own = hold_rate * vec[row, half:] + jnp.where(me == 0, low, high)
        own = vec[row, :half] - learn_rate * new_own
        new_other = hold_rate * got_vec[row, half:] + jnp.where(me == 0, high, low)
        other = got_vec[row, :half] - learn_rate * new_other
        state[...] = new_own.reshape(state.shape)
        stepped[...] = own.reshape(stepped.shape)
        whole = jnp.concatenate(
            [jnp.where(me == 0, own, other), jnp.where(me == 0, other, own)], axis=1
        )
        rounded[...] = whole.reshape(rounded.shape).astype(rounded.dtype)

    @pl.when(me == 0)
    def _():
        wait_for(sum_d.at[last, :], part_sem.at[groups + 3])
        sum_columns(last, None, own_d, sum_d, sum_d)
        wait_for(pack.at[0], more_sem.at[1])

    @pl.when(me == 1)
    def _():
        wait_for(pack.at[0, head, :], more_sem.at[1])

    wait_for(base_d, more_sem.at[4])

    send_vec.wait_send()
    wait_for(stat_u.at[pl.ds(0, gathered * (n - 1))], small_sem.at[1])
    wait_for(stat_w.at[pl.ds(0, (groups - gathered) * (2 * n - 1))], small_sem.at[2])
    wait_for(stat_d.at[pl.ds(0, 2 * n - 1)], small_sem.at[3])
    wait_for(stat_m.at[pl.ds(0, 2 * n - 1)], small_sem.at[5])
    wait_for(stat_m.at[pl.ds(0, 2 * n - 1)], stat_sem.at[groups + 1])
    wait_for(cu.at[at_core(peer, rows, 0, first), :], more_sem.at[3])
    wait_for(pack, send_sem.at[0])
    wait_for(stat_d.at[pl.ds(0, 2 * n - 1)], stat_sem.at[groups])

    @pl.when(me == 0)
    def _():
        wait_for(stat_o, stat_sem.at[groups + 2])

    @pl.when(me == 1)
    def _():
        wait_for(stat_o.at[pl.ds(0, n - 1)], stat_sem.at[groups + 2])
        wait_for(stat_d.at[pl.ds(0, 2 * n - 1)], small_sem.at[6])


def finish(
    cu_v, cn_v, cb_v, su_v, sn_v, sb_v, tu_v, tn_v, tb_v,
    pack, ed, stat_d, stat_m, stat_o,
    cu, cd, cn, cb, su, sd, sn, sb, tu, td, tn, tb,
    cd_v, sd_v, td_v,
):
    me = lax.axis_index("dp")
    rate = lax.axis_size("dp") ** (-0.5)
    n = lax.axis_size("tp")
    tall, cols = td_v.shape
    step = 32
    mine_d, base_o, sum_d, base_d, give_d = (pack.at[at] for at in range(5))

    def out(source, target, sem):
        copy = pltpu.make_async_copy(source, target, sem)
        copy.start()
        return copy

    def write(sem):
        small = [
            pltpu.make_async_copy(source, target, sem.at[2 + at])
            for at, (source, target) in enumerate(
                ((cn_v, cn), (cb_v, cb), (sn_v, sn), (sb_v, sb), (tn_v, tn), (tb_v, tb))
            )
        ]
        for copy in small:
            copy.start()
        matrices(sem)
        for copy in small:
            copy.wait()
        wait_for(cu_v, sem.at[1])
        wait_for(pack, sem.at[0])

    def matrices(sem):
        out(su_v, su, sem.at[0])
        out(tu_v, tu, sem.at[0])
        out(cu_v, cu, sem.at[1])

        scales = []
        for core in (me, 1 - me):
            weights = sizes = 0.0
            for at in range(n):
                weights = weights + stat_m[core * n + at]
                sizes = sizes + stat_d[core * n + at] + jnp.where(core == 0, stat_o[at], 0.0)
            scales.append(scale_of(weights, sizes, rate))
        own, other = scales
        for piece in range(pieces):
            size = tall // pieces

            @blocks(size, step)
            def _(at):
                span = pl.ds(pl.multiple_of(piece * size + at, step), step)
                x = sum_d[span, :] * own
                td_v[span, :] = hold_rate * ed[span, :] + x
                stepped = base_d[span, :] - learn_rate * x
                sd_v[span, :] = stepped
                cd_v[span, pl.ds(pl.multiple_of(me * cols, cols), cols)] = stepped.astype(cd_v.dtype)
                x = (give_d[span, :] + mine_d[span, :]) * other
                stepped = base_o[span, :] - learn_rate * x
                cd_v[span, pl.ds(pl.multiple_of((1 - me) * cols, cols), cols)] = stepped.astype(cd_v.dtype)

            span = pl.ds(piece * size, size)
            out(td_v.at[span, :], td.at[span, :], sem.at[0])
            out(sd_v.at[span, :], sd.at[span, :], sem.at[0])
            out(cd_v.at[span, :], cd.at[span, :], sem.at[0])

    pl.run_scoped(write, pltpu.SemaphoreType.DMA((8,)))


def held(arrays):
    return [pltpu.with_memory_space_constraint(x, pltpu.HBM) for x in arrays]


def on_pair(*args):
    pu, pd, pn, pb, mu, md, mn, mb, eu, ed, en, eb = args
    n = lax.axis_size("tp")
    f32, bf16 = jnp.float32, jnp.bfloat16
    vmem = pl.BlockSpec(memory_space=pltpu.VMEM)
    hbm = pl.BlockSpec(memory_space=pltpu.HBM)
    wide, tall = pu.shape[2], pd.shape[1]
    rows, cols = mu.shape[0], md.shape[1]
    groups = rows // lanes
    rest = rows - gathered * lanes

    def shaped(shape, dtype=f32):
        return jax.ShapeDtypeStruct(shape, dtype)

    between = [
        shaped((pu.shape[1], wide), bf16), shaped((pn.shape[1],), bf16), shaped((pb.shape[1],), bf16),
        *(shaped(x.shape) for x in (mu, mn, mb)),
        *(shaped(x.shape) for x in (mu, mn, mb)),
        shaped((5, *md.shape)),
        shaped(md.shape),
        shaped((2 * n, 1, cols)),
        shaped((2 * n, 1, cols)),
        shaped((n, 1, cols)),
    ]
    results = pl.pallas_call(
        exchange,
        out_shape=between,
        in_specs=[hbm] * len(args),
        out_specs=[vmem] * len(between),
        scratch_shapes=[
            pltpu.VMEM(mu.shape, f32),
            pltpu.VMEM(md.shape, f32),
            pltpu.VMEM((rest, wide), f32),
            pltpu.VMEM(mu.shape, f32),
            pltpu.VMEM((rest, wide), f32),
            pltpu.VMEM((2, rest, wide), f32),
            *(pltpu.VMEM(x.shape, f32) for x in (mu, md, mu)),
            *(pltpu.VMEM(x.shape, f32) for x in (pn, pb, mn, mb, en, eb)),
            pltpu.VMEM((4, pn.shape[1]), f32),
            pltpu.VMEM((4, pn.shape[1]), f32),
            pltpu.VMEM((rows, lanes), f32),
            pltpu.VMEM((rest, lanes), f32),
            pltpu.VMEM((8, cols), f32),
            pltpu.VMEM((8, cols), f32),
            pltpu.VMEM((gathered * n, 2, lanes), f32),
            pltpu.VMEM(((groups - gathered) * 2 * n, 2, lanes), f32),
        ],
        compiler_params=pltpu.CompilerParams(
            collective_id=0, has_side_effects=True, vmem_limit_bytes=40 * 2**20
        ),
        name="exchange",
    )(*held((pu[0], pd[0], *args[2:])))
    outs = (
        ((pu.shape[1], wide), bf16),
        ((tall, pd.shape[2]), bf16),
        ((pn.shape[1],), bf16),
        ((pb.shape[1],), bf16),
        *((x.shape, f32) for x in (mu, md, mn, mb)),
        *((x.shape, f32) for x in (mu, md, mn, mb)),
    )
    return tuple(pl.pallas_call(
        finish,
        out_shape=[shaped(shape, dtype) for shape, dtype in outs],
        in_specs=[vmem] * len(between),
        out_specs=[hbm] * len(outs),
        scratch_shapes=[
            pltpu.VMEM((tall, pd.shape[2]), bf16),
            pltpu.VMEM(md.shape, f32),
            pltpu.VMEM(md.shape, f32),
        ],
        compiler_params=pltpu.CompilerParams(vmem_limit_bytes=8 * 2**20),
        name="finish",
    )(*results))


def solution(mesh):
    in_specs = (
        P(("job", "dp"), None, "tp"),
        P(("job", "dp"), "tp", None),
        P(("job", "dp"), None),
        P(("job", "dp"), None),
        P(("job", "dp"), "tp"),
        P(("job", "tp"), "dp"),
        P(("job", "dp")),
        P(("job", "dp")),
        P(("job", "dp"), "tp"),
        P(("job", "tp"), "dp"),
        P(("job", "dp")),
        P(("job", "dp")),
    )
    out_specs = (
        P("job", "tp"),
        P(("job", "tp"), None),
        P("job"),
        P("job"),
        P(("job", "dp"), "tp"),
        P(("job", "tp"), "dp"),
        P(("job", "dp")),
        P(("job", "dp")),
        P(("job", "dp"), "tp"),
        P(("job", "tp"), "dp"),
        P(("job", "dp")),
        P(("job", "dp")),
    )
    return jax.shard_map(
        on_device if mesh.shape["dp"] != 2 else on_pair, mesh=mesh, in_specs=in_specs, out_specs=out_specs, check_vma=False
    )
```
